32 devices in a mesh: fsdp: 16 (over z, y, core), tp: 2 (over x).
Axes of the slice: x: 2, y: 2, z: 4, core: 2. Of those that a mesh axis runs over, the one named last changes fastest.
Arguments:
- tokens: bfloat16 [6144, 5632], P('fsdp', 'tp'), may hold values from -6 to 6
- gain: float32 [5632], replicated, may hold values from 0.1 to 1.9
- query_projection_weight: bfloat16 [5632, 6144], P('fsdp', 'tp'), may hold values from -0.078125 to 0.078125
- key_projection_weight: bfloat16 [5632, 1024], P('fsdp', 'tp'), may hold values from -0.078125 to 0.078125
- value_projection_weight: bfloat16 [5632, 1024], P('fsdp', 'tp'), may hold values from -0.078125 to 0.078125
- adapter_down_factors: bfloat16 [3, 16, 5632], replicated, may hold values from -0.078125 to 0.078125
- query_adapter_up: bfloat16 [16, 6144], P(None, 'tp'), may hold values from -0.078125 to 0.078125
- key_adapter_up: bfloat16 [16, 1024], P(None, 'tp'), may hold values from -0.1875 to 0.1875
- value_adapter_up: bfloat16 [16, 1024], P(None, 'tp'), may hold values from -0.1875 to 0.1875
- query_cotangent: bfloat16 [6144, 6144], P('fsdp', 'tp'), may hold values from -6 to 6
- key_cotangent: bfloat16 [6144, 1024], P('fsdp', 'tp'), may hold values from -6 to 6
- value_cotangent: bfloat16 [6144, 1024], P('fsdp', 'tp'), may hold values from -6 to 6
Outputs:
- grad_tokens: bfloat16 [6144, 5632], P('fsdp', 'tp')
- grad_down: float32 [3, 16, 5632], P(None, None, 'tp')
- grad_up_query: float32 [16, 6144], P(None, 'tp')
- grad_up_key: float32 [16, 1024], P(None, 'tp')
- grad_up_value: float32 [16, 1024], P(None, 'tp')
The draws below stay inside these ranges and needn't reach their ends.
All inputs are finite; a program needn't handle non-finite values.
Results may differ from the reference program's by a relative error of at most 0.0096.
Values may be sent and summed in bfloat16 or wider, within the bound.
A program may use at most 128 MiB of HBM per device.

```python
import math
import jax
import jax.numpy as jnp
from jax import lax

MODEL_WIDTH = 5632
ADAPTER_RANK = 16
QUERY_WIDTH = 6144
KEY_VALUE_WIDTH = 1024
TOKEN_TOTAL = 6144


def steps_of(stream_key, dims, pieces, low, largest):
    factor_of = 1.0
    for dim, blocks in pieces:
        draws = jax.random.uniform(jax.random.fold_in(jax.random.fold_in(stream_key, 6), dim), (blocks,), jnp.float32, low / len(pieces), largest / len(pieces))
        factor_of = factor_of * jnp.repeat(jnp.exp(draws), dims[dim] // blocks).reshape((-1,) + (1,) * (len(dims) - 1 - dim))
    return factor_of


def scatter_about(key, extent, scale, most, split=(), kind=jnp.bfloat16):
    level = steps_of(key, extent, split, -0.22, 0.18) if split else 1.0
    drawn = jax.random.normal(key, extent, jnp.float32) * scale * level
    return jnp.minimum(jnp.maximum(drawn, -most), most).astype(kind)


def setup_inputs(seed: int = 0) -> dict:
    splits = jax.random.split(jax.random.key(seed), 13)
    return {
        "tokens": scatter_about(splits[0], (TOKEN_TOTAL, MODEL_WIDTH), 1.0, 6.0, ((0, 16), (1, 2))),
        "gain": jnp.clip(1.0 + 0.18 * jax.random.normal(splits[1], (MODEL_WIDTH,), jnp.float32), 0.1, 1.9),
        "query_projection_weight": scatter_about(splits[2], (MODEL_WIDTH, QUERY_WIDTH), MODEL_WIDTH ** -0.5, 0.078125, ((0, 16), (1, 2))),
        "key_projection_weight": scatter_about(splits[3], (MODEL_WIDTH, KEY_VALUE_WIDTH), MODEL_WIDTH ** -0.5, 0.078125, ((0, 16), (1, 2))),
        "value_projection_weight": scatter_about(splits[4], (MODEL_WIDTH, KEY_VALUE_WIDTH), MODEL_WIDTH ** -0.5, 0.078125, ((0, 16), (1, 2))),
        "adapter_down_factors": scatter_about(splits[5], (3, ADAPTER_RANK, MODEL_WIDTH), MODEL_WIDTH ** -0.5, 0.078125),
        "query_adapter_up": scatter_about(splits[6], (ADAPTER_RANK, QUERY_WIDTH), QUERY_WIDTH ** -0.5, 0.078125, ((1, 2),)),
        "key_adapter_up": scatter_about(splits[7], (ADAPTER_RANK, KEY_VALUE_WIDTH), KEY_VALUE_WIDTH ** -0.5, 0.1875, ((1, 2),)),
        "value_adapter_up": scatter_about(splits[8], (ADAPTER_RANK, KEY_VALUE_WIDTH), KEY_VALUE_WIDTH ** -0.5, 0.1875, ((1, 2),)),
        "query_cotangent": scatter_about(splits[9], (TOKEN_TOTAL, QUERY_WIDTH), 1.0, 6.0, ((0, 16), (1, 2))),
        "key_cotangent": scatter_about(splits[10], (TOKEN_TOTAL, KEY_VALUE_WIDTH), 1.0, 6.0, ((0, 16), (1, 2))),
        "value_cotangent": scatter_about(splits[11], (TOKEN_TOTAL, KEY_VALUE_WIDTH), 1.0, 6.0, ((0, 16), (1, 2))),
    }


norm_eps = 1e-05
adapter_scale = 2.0

def reference(tokens, gain, query_projection_weight, key_projection_weight, value_projection_weight, adapter_down_factors, query_adapter_up, key_adapter_up, value_adapter_up, query_cotangent, key_cotangent, value_cotangent):
    weights = (query_projection_weight, key_projection_weight, value_projection_weight)
    adapter_up_factors = (query_adapter_up, key_adapter_up, value_adapter_up)
    cotangent_list = (query_cotangent, key_cotangent, value_cotangent)
    token_width_matrix = tokens.astype(jnp.float32)
    inverse_root_mean = lax.rsqrt(lax.optimization_barrier(jnp.mean(token_width_matrix * token_width_matrix, axis=1, keepdims=True)) + norm_eps)
    unit_rows = token_width_matrix * inverse_root_mean
    scaled_input = unit_rows * gain[None, :]
    normed = scaled_input.astype(jnp.bfloat16)
    adapter_input = jnp.stack([jnp.dot(scaled_input, adapter_down_factors[slice_member].astype(jnp.float32).T, precision=lax.Precision.HIGHEST) for slice_member in range(3)])
    adapter_output = jnp.stack([jnp.dot(cotangent_list[slice_member], adapter_up_factors[slice_member].T, preferred_element_type=jnp.float32) for slice_member in range(3)])
    input_lowrank = adapter_input.astype(jnp.bfloat16)
    output_lowrank = adapter_output.astype(jnp.bfloat16)
    gradient_scale = adapter_scale / math.sqrt(TOKEN_TOTAL)
    backward_result = jnp.zeros(tokens.shape, jnp.float32)
    for slice_member in range(3):
        backward_result = backward_result + jnp.dot(cotangent_list[slice_member], weights[slice_member].T, preferred_element_type=jnp.float32)
    for slice_member in range(3):
        backward_result = backward_result + adapter_scale * jnp.dot(output_lowrank[slice_member], adapter_down_factors[slice_member], preferred_element_type=jnp.float32)
    gained = gain[None, :] * backward_result
    inner = lax.optimization_barrier(jnp.mean(gained * unit_rows, axis=1, keepdims=True))
    grad_tokens = (inverse_root_mean * (gained - unit_rows * inner)).astype(jnp.bfloat16)
    grad_down = jnp.stack([gradient_scale * jnp.dot(output_lowrank[slice_member].T, normed, preferred_element_type=jnp.float32) for slice_member in range(3)])
    grad_ups = [gradient_scale * jnp.dot(input_lowrank[slice_member].T, cotangent_list[slice_member], preferred_element_type=jnp.float32) for slice_member in range(3)]
    return (grad_tokens, grad_down, grad_ups[0], grad_ups[1], grad_ups[2])
```

```python
import functools
import math

import jax
import jax.numpy as jnp
from jax import lax
from jax.experimental import pallas as pl
from jax.experimental.pallas import tpu as pltpu
from jax.sharding import PartitionSpec as P

norm_eps = 1e-05
adapter_scale = 2.0


def transposed_product(left, right):
    return lax.dot_general(
        left, right, (((1,), (1,)), ((), ())), preferred_element_type=jnp.float32
    )


def plain_back(weights, cotangents, full_width):
    total = jnp.zeros((cotangents[0].shape[0], full_width), jnp.float32)
    for weight, cotangent in zip(weights, cotangents):
        whole = lax.all_gather(weight, "fsdp", axis=0, tiled=True)
        total = total + transposed_product(cotangent, whole)
    return lax.psum_scatter(total, "tp", scatter_dimension=1, tiled=True)


def near_and_far_orders(count):
    near = range(count)
    outer, outer_marks = [], {}
    inner, inner_marks = [], {}

    def add(order, marks, name, tiles):
        marks[name] = len(order)
        order.extend(tiles)

    def grid(ws, ts):
        return [(w, t) for w in ws for t in ts]

    add(outer, outer_marks, "near", grid((0, 1), near))
    add(outer, outer_marks, "f0", grid((4,), near))
    add(outer, outer_marks, "y", grid((2, 3), near))
    add(outer, outer_marks, "f1", grid((5,), near))
    done = [0, 1, 2, 3, 4, 5]
    for i in range(count):
        add(outer, outer_marks, f"z{i}", grid(done, (count + i,)))
        if i >= count - 3 and i < count - 1:
            w = 6 + i - (count - 3)
            add(outer, outer_marks, f"fy{w - 6}", grid((w,), range(count + i + 1)))
            done.append(w)
    every = range(2 * count)
    add(inner, inner_marks, "near", grid((0, 1), near))
    for i in range(count):
        add(inner, inner_marks, f"z{i}", grid((0, 1), (count + i,)))
    add(inner, inner_marks, "y", grid((2, 3), every))
    add(inner, inner_marks, "f0", grid((4,), every))
    add(inner, inner_marks, "fy0", grid((6,), every))
    add(inner, inner_marks, "f1", grid((5,), every))
    add(inner, inner_marks, "fy1", grid((7,), every))
    return (outer, outer_marks), (inner, inner_marks)


def packed(digits):
    words = []
    for low in range(0, len(digits), 10):
        words.append(sum(d << (3 * k) for k, d in enumerate(digits[low : low + 10])))
    return words


def digit_at(step, is_inner, outer_digits, inner_digits):
    word = jnp.int32(0)
    for k, (o, i) in enumerate(zip(packed(outer_digits), packed(inner_digits))):
        value = jnp.where(is_inner == 1, jnp.int32(i), jnp.int32(o))
        word = jnp.where(step // 10 == k, value, word)
    return lax.shift_right_logical(word, 3 * (step % 10)) % 8


def piece_rows(half):
    size = 48 if half > 48 else half
    cuts = list(range(0, half, size)) + [half]
    return list(zip(cuts[:-1], cuts[1:]))


def grid_kernel(
    settings,
    cq, ck, cv, wq, wk, wv, tokens, gain, adapters, uq, uk, uv,
    out, grad_down, grad_up_q, grad_up_k, grad_up_v,
    W, C, S, X, R,
    T, GA, U, D, GD, A, AR, INV, LO, ZT, N, B, I, IR,
    G, GC, GY, H, HZ, F,
    load_w, load_c, load_s,
    a_send, a_recv, i_send, i_recv,
    gc_send, gc_recv, gy_send, gy_recv, gz_send, gz_recv, ga_send, ga_recv, gb_send, gb_recv, gd_send, gd_recv,
    cc_send, cc_recv, cz_send, cz_recv, zc_send, zc_recv,
    y_send, y_recv, far_send, far_recv, fy_send, fy_recv,
    x_send, x_recv, r_send, r_recv,
):
    half = W.shape[1]
    block = 2 * half
    count = C.shape[0] // 2
    lanes = R.shape[2]
    top = 8
    place = lax.axis_index("fsdp")
    side = lax.axis_index("tp")

    def flipped(bit):
        return place + bit * (1 - 2 * ((place // bit) % 2))

    def at(bit):
        return {"fsdp": flipped(bit), "tp": side}

    def both(one, two):
        return {"fsdp": flipped(one) + flipped(two) - place, "tp": side}

    core, row, near_z, far_z = at(1), at(2), at(4), at(8)
    diagonal, third_z = both(4, 1), both(4, 8)
    twin = {"fsdp": place, "tp": 1 - side}
    z = place // 4
    is_inner = ((z + 1) // 2) % 2
    keep_late = (place // top + side) % 2

    pieces = piece_rows(half)
    columns = []
    low = 0
    for ref in (cq, ck, cv):
        columns.append((low, low + ref.shape[1]))
        low += ref.shape[1]

    def load_cot(i, m):
        low, high = columns[m]
        ref = (cq, ck, cv)[m]
        return pltpu.make_async_copy(
            ref.at[pl.ds(i * lanes, lanes), :],
            C.at[i, pl.ds(0, lanes), pl.ds(low, high - low)],
            load_c.at[i, m],
        )

    def load_weight(h, m):
        low, high = columns[m]
        ref = (wq, wk, wv)[m]
        return pltpu.make_async_copy(
            ref.at[pl.ds(h * half, half), :],
            W.at[h, :, pl.ds(low, high - low)],
            load_w.at[h, m],
        )

    def remote(src, dst, send, recv, device):
        return pltpu.make_async_remote_copy(
            src_ref=src, dst_ref=dst, send_sem=send, recv_sem=recv,
            device_id=device, device_id_type=pl.DeviceIdType.MESH,
        )

    lower, upper = pl.ds(0, lanes), pl.ds(lanes, lanes)
    full_width, owned, rank, scale = settings
    own_columns = pl.ds(pl.multiple_of(side * owned, lanes), owned)
    feature_blocks = owned // lanes
    share = F.shape[0] // 2
    core_index, row_index = place % 2, (place // 2) % 2
    part_start = core_index * share + row_index * (share // 2)
    piece = share // 8

    small_loads = [
        pltpu.make_async_copy(tokens, T, load_s.at[0]),
        pltpu.make_async_copy(gain.at[:, own_columns], GA, load_s.at[1]),
    ]
    for m in range(3):
        small_loads.append(
            pltpu.make_async_copy(
                adapters.at[m, :, own_columns], D.at[pl.ds(rank * m, rank)], load_s.at[2 + m]
            )
        )
        low, high = columns[m]
        small_loads.append(
            pltpu.make_async_copy(
                (uq, uk, uv)[m],
                U.at[pl.ds(rank * m, rank), pl.ds(low, high - low)],
                load_s.at[5 + m],
            )
        )

    def pair_rows():
        return remote(A, AR, a_send, a_recv, twin)

    def inner_rows(i):
        return remote(I.at[i], IR.at[i], i_send, i_recv.at[i], twin)

    def grads_core():
        away = (1 - core_index) * share
        return remote(G.at[pl.ds(away, share)], GC, gc_send, gc_recv, core)

    def grads_row():
        away = core_index * share + (1 - row_index) * (share // 2)
        return remote(G.at[pl.ds(away, share // 2)], GY, gy_send, gy_recv, row)

    z_partners = ((near_z, 1), (far_z, 2), (third_z, 3))

    def z_flip(bits):
        low, high = z % 2, z // 2
        low = 1 - low if bits % 2 else low
        high = 1 - high if bits // 2 else high
        return 2 * high + low

    def grads_z(n):
        device, bits = z_partners[n]
        return remote(
            H.at[pl.ds(z_flip(bits) * piece, piece)], HZ.at[n], gz_send, gz_recv.at[n], device
        )

    mine_z = pl.ds(part_start + z * piece, piece)
    mine_y = pl.ds(part_start, share // 2)
    mine_c = pl.ds(core_index * share, share)

    def spread_z(n):
        return remote(F.at[mine_z], F.at[mine_z], ga_send, ga_recv.at[n], z_partners[n][0])

    def spread_y():
        return remote(F.at[mine_y], F.at[mine_y], gb_send, gb_recv, row)

    def spread_c():
        return remote(F.at[mine_c], F.at[mine_c], gd_send, gd_recv, core)

    def cot_core(i):
        return remote(C.at[i, lower], C.at[i, upper], cc_send, cc_recv.at[i], core)

    def cot_z(i):
        return remote(C.at[i, lower], C.at[count + i, lower], cz_send, cz_recv.at[i], near_z)

    def cot_zc(i):
        return remote(
            C.at[count + i, lower], C.at[count + i, upper], zc_send, zc_recv.at[i], core
        )

    def weight_y(h):
        return remote(W.at[h], W.at[2 + h], y_send, y_recv.at[h], row)

    def far(h, k):
        low, high = pieces[k]
        rows = pl.ds(low, high - low)
        return remote(W.at[h, rows], W.at[4 + h, rows], far_send, far_recv.at[h, k], far_z)

    def far_y(h, k):
        low, high = pieces[k]
        rows = pl.ds(low, high - low)
        return remote(W.at[4 + h, rows], W.at[6 + h, rows], fy_send, fy_recv.at[h, k], row)

    for i in range(count):
        for m in range(3):
            load_cot(i, m).start()
    for h in range(2):
        for m in range(3):
            load_weight(h, m).start()
    for copy in small_loads:
        copy.start()

    barrier = pltpu.get_barrier_semaphore()
    partners = (core, row, near_z, diagonal, far_z, third_z, twin)
    for partner in partners:
        pl.semaphore_signal(
            barrier, inc=1, device_id=partner, device_id_type=pl.DeviceIdType.MESH
        )
    pl.semaphore_wait(barrier, len(partners))

    for i in range(count):
        for m in range(3):
            load_cot(i, m).wait()

        @pl.when(is_inner == 0)
        def _():
            cot_z(i).start()

    for h in range(2):
        for m in range(3):
            load_weight(h, m).wait()

        @pl.when(is_inner == 1)
        def _():
            for k in range(len(pieces)):
                far(h, k).start()

        if h == 0:
            weight_y(h).start()
    for i in range(count):
        cot_core(i).start()

    lane = lax.broadcasted_iota(jnp.int32, (lanes, lanes), 1)
    used = 3 * rank
    D[pl.ds(used, lanes - used), :] = jnp.zeros((lanes - used, owned), jnp.bfloat16)
    U[pl.ds(used, lanes - used), :] = jnp.zeros((lanes - used, U.shape[1]), jnp.bfloat16)
    for m in range(3):
        for other in range(3):
            if other != m:
                low, high = columns[other]
                U[pl.ds(rank * m, rank), pl.ds(low, high - low)] = jnp.zeros(
                    (rank, high - low), jnp.bfloat16
                )
    for p in range(3):
        GD[p] = jnp.zeros((lanes, owned), jnp.bfloat16)
    for copy in small_loads:
        copy.wait()
    rest = D[pl.ds(0, used), :].astype(jnp.float32) * GA[...]
    for p in range(3):
        part = rest.astype(jnp.bfloat16)
        GD[p, pl.ds(64, used), :] = part
        rest = rest - part.astype(jnp.float32)

    def nt_dot(left, right):
        return lax.dot_general(
            left, right, (((1,), (1,)), ((), ())), preferred_element_type=jnp.float32
        )

    for i in range(count):
        rows = pl.ds(i * lanes, lanes)
        own_rows = T[rows, :]
        value = nt_dot(C[i, lower, :], U[...])
        for p in range(3):
            value = value + nt_dot(own_rows, GD[p])
        wide = own_rows.astype(jnp.float32)
        squares = jnp.sum(wide * wide, axis=1, keepdims=True)
        A[i] = value + jnp.where(lane == 120, squares, 0.0)
    pair_rows().start()
    pair_rows().wait_recv()
    for i in range(count):
        rows = pl.ds(i * lanes, lanes)
        both_sum = A[i] + AR[i]
        squares = jnp.sum(jnp.where(lane == 120, both_sum, 0.0), axis=1, keepdims=True)
        inverse = lax.rsqrt(squares / full_width + norm_eps)
        INV[i] = jnp.broadcast_to(inverse, (lanes, lanes))
        low = jnp.where(lane < used, both_sum, 0.0)
        LO[i] = low.astype(jnp.bfloat16)
        scaled = jnp.where((lane >= 64) & (lane < 64 + used), both_sum * inverse, 0.0)
        ZT[:, rows] = (low + scaled).T.astype(jnp.bfloat16)
        N[rows, :] = (T[rows, :].astype(jnp.float32) * inverse * GA[...]).astype(jnp.bfloat16)

    def down_block(j, carry):
        cols = pl.ds(pl.multiple_of(j * lanes, lanes), lanes)
        value = scale * jnp.dot(
            ZT[pl.ds(0, 64), :], N[:, cols], preferred_element_type=jnp.float32
        )
        for m in range(3):
            G[m * feature_blocks + j] = value[rank * m : rank * (m + 1)]
        return carry

    lax.fori_loop(0, feature_blocks, down_block, 0)
    first = 3 * feature_blocks
    for m in range(3):
        low, high = columns[m]

        def up_block(j, carry, m=m, low=low):
            cols = pl.ds(pl.multiple_of(low + j * lanes, lanes), lanes)
            value = jnp.zeros((rank, lanes), jnp.float32)
            for i in range(count):
                value = value + jnp.dot(
                    ZT[pl.ds(64 + rank * m, rank), pl.ds(i * lanes, lanes)],
                    C[i, lower, cols],
                    preferred_element_type=jnp.float32,
                )
            G[first + low // lanes + j] = scale * value
            return carry

        lax.fori_loop(0, (high - low) // lanes, up_block, 0)
    filled = first + columns[2][1] // lanes
    for j in range(filled, G.shape[0]):
        G[j] = jnp.zeros((rank, lanes), jnp.float32)
    grads_core().start()
    grads_core().wait_recv()
    G[mine_c] = G[mine_c] + GC[...]
    grads_row().start()
    weight_y(1).start()

    (outer, outer_marks), (inner, inner_marks) = near_and_far_orders(count)
    tiles = len(outer)
    lag = 4

    def order_at(step):
        w = digit_at(step, is_inner, [a for a, _ in outer], [a for a, _ in inner])
        t = digit_at(step, is_inner, [b for _, b in outer], [b for _, b in inner])
        return w, t

    def when(step, outer_name, inner_name):
        o = outer_marks[outer_name] if outer_name else -1
        i = inner_marks[inner_name] if inner_name else -1
        return pl.when(step == is_inner * i + (1 - is_inner) * o)

    def take_far(h, k):
        far(h, k).wait_recv()
        far_y(h, k).start()

    def body(step, carry):
        @when(step, "near", "near")
        def _():
            for i in range(count):
                cot_core(i).wait_recv()

        @when(step, None, f"z{count - 1}")
        def _():
            remote(W.at[pl.ds(0, 2)], W.at[pl.ds(4, 2)], far_send, far_recv.at[0, 0], far_z).wait_send()
            for i in range(count - 1):
                cot_z(i).start()

        @when(step, "f0", "z1")
        def _():
            grads_row().wait_recv()
            G[mine_y] = G[mine_y] + GY[...]
            H[...] = G[mine_y].astype(jnp.bfloat16)
            for n in range(3):
                grads_z(n).start()

        @when(step, "y", None)
        def _():
            for k in range(len(pieces)):
                far(0, k).start()

        @when(step, "z0", "f0")
        def _():
            value = G[mine_z]
            for n in range(3):
                grads_z(n).wait_recv()
                value = value + HZ[n].astype(jnp.float32)
            F[mine_z] = value.astype(jnp.bfloat16)
            for n in range(3):
                spread_z(n).start()

        @when(step, "z0", None)
        def _():
            for k in range(len(pieces)):
                far(1, k).start()

        @when(step, None, "f0")
        def _():
            cot_z(count - 1).start()

        @when(step, "fy1", "f1")
        def _():
            for n in range(3):
                spread_z(n).wait_recv()
            spread_y().start()

        for i in range(count):
            @when(step, f"z{i}", f"z{i}")
            def _():
                cot_z(i).wait_recv()
                cot_zc(i).start()
                cot_zc(i).wait_recv()

        @when(step, "y", "y")
        def _():
            weight_y(0).wait_recv()
            weight_y(1).wait_recv()

        number = len(pieces)

        @when(step, "f0", "f0")
        def _():
            for k in range(number):
                take_far(0, k)

        split = number // 2

        @when(step, "f1", "fy0")
        def _():
            for k in range(split):
                take_far(1, k)

        @when(step, "f1", "f1")
        def _():
            for k in range(split, number):
                take_far(1, k)

        for h in range(2):
            @when(step, f"fy{h}", f"fy{h}")
            def _():
                for k in range(number):
                    far_y(h, k).wait_recv()

        w, t = order_at(step)

        @pl.when(step < tiles)
        def _():
            value = lax.dot_general(
                W[w], C[t], (((1,), (1,)), ((), ())), preferred_element_type=jnp.float32
            ).astype(jnp.bfloat16)
            S[w, t, 0] = value[:, :lanes]
            S[w, t, 1] = value[:, lanes:]

        @pl.when((step < tiles) & (w // 4 != keep_late))
        def _():
            remote(S.at[w, t], X.at[w % 4, t], x_send, x_recv.at[w % 4, t], twin).start()

        back = jnp.maximum(step - lag, 0)
        w2, t2 = order_at(back)

        @pl.when((step >= lag) & (w2 // 4 == keep_late))
        def _():
            remote(S.at[w2, t2], X.at[w2 % 4, t2], x_send, x_recv.at[w2 % 4, t2], twin).wait_recv()
            total = S[w2, t2].astype(jnp.float32) + X[w2 % 4, t2].astype(jnp.float32)
            S[w2, t2] = total.astype(jnp.bfloat16)
            base = place % top
            index = base + ((w2 // 2) % 2) * 2 * (1 - 2 * ((base // 2) % 2))
            rows = pl.ds(pl.multiple_of(index * block + (w2 % 2) * half, 16), half)
            i = t2 % count

            @pl.when(t2 < count)
            def _():
                R[i, rows, :] = total[0].astype(jnp.bfloat16)
                remote(S.at[w2, t2, 1], R.at[i, rows], r_send, r_recv, core).start()

            @pl.when(t2 >= count)
            def _():
                remote(S.at[w2, t2, 0], R.at[i, rows], r_send, r_recv, near_z).start()
                remote(S.at[w2, t2, 1], R.at[i, rows], r_send, r_recv, diagonal).start()

        return carry

    lax.fori_loop(0, tiles + lag, body, 0)

    spread_y().wait_recv()
    spread_c().start()
    part = pl.ds(0, 3 * R.shape[1] // 4)
    results = remote(R.at[:, part], R.at[:, part], r_send, r_recv, core)
    results.wait_recv()
    for i in range(count):
        rows = pl.ds(i * lanes, lanes)

        def gained_block(j, carry, i=i, rows=rows):
            cols = pl.ds(pl.multiple_of(j * lanes, lanes), lanes)
            back = R[i, cols, :].astype(jnp.float32).T
            back = back + adapter_scale * jnp.dot(
                LO[i], D[:, cols], preferred_element_type=jnp.float32
            )
            gained = GA[:, cols] * back
            B[rows, cols] = gained
            return carry + gained * (T[rows, cols].astype(jnp.float32) * INV[i])

        total = lax.fori_loop(0, feature_blocks, gained_block, jnp.zeros((lanes, lanes), jnp.float32))
        I[i] = jnp.broadcast_to(jnp.sum(total, axis=1, keepdims=True), (lanes, lanes))
        inner_rows(i).start()
    spread_c().wait_recv()
    for j in range(feature_blocks):
        for m in range(3):
            grad_down[m, :, pl.ds(j * lanes, lanes)] = F[m * feature_blocks + j].astype(jnp.float32)
    for m, ref in enumerate((grad_up_q, grad_up_k, grad_up_v)):
        low, high = columns[m]
        for j in range((high - low) // lanes):
            ref[:, pl.ds(j * lanes, lanes)] = F[first + low // lanes + j].astype(jnp.float32)
    for i in range(count):
        rows = pl.ds(i * lanes, lanes)
        inner_rows(i).wait_recv()
        inner = (I[i] + IR[i]) / full_width

        def final_block(j, carry, i=i, rows=rows, inner=inner):
            cols = pl.ds(pl.multiple_of(j * lanes, lanes), lanes)
            unit = T[rows, cols].astype(jnp.float32) * INV[i]
            out[rows, cols] = (INV[i] * (B[rows, cols] - unit * inner)).astype(jnp.bfloat16)
            return carry

        lax.fori_loop(0, feature_blocks, final_block, 0)

    results.wait_send()
    own = C.at[pl.ds(0, count), lower]
    remote(own, own, cc_send, cc_recv.at[0], core).wait_send()
    remote(own, own, cz_send, cz_recv.at[0], core).wait_send()
    remote(own, own, zc_send, zc_recv.at[0], core).wait_send()
    two = W.at[pl.ds(0, 2)]
    remote(two, two, y_send, y_recv.at[0], core).wait_send()

    @pl.when(is_inner == 0)
    def _():
        remote(two, two, far_send, far_recv.at[0, 0], core).wait_send()

    remote(two, two, fy_send, fy_recv.at[0, 0], core).wait_send()
    four = S.at[pl.ds(0, 4)]
    remote(four, four, x_send, x_recv.at[0, 0], core).wait_send()
    pair_rows().wait_send()
    remote(I, I, i_send, i_recv.at[0], twin).wait_send()
    grads_core().wait_send()
    grads_row().wait_send()
    three = H.at[pl.ds(0, 3 * piece)]
    remote(three, three, gz_send, gz_recv.at[0], core).wait_send()
    three = F.at[pl.ds(0, 3 * piece)]
    remote(three, three, ga_send, ga_recv.at[0], core).wait_send()
    spread_y().wait_send()
    spread_c().wait_send()


token_lanes = 128


def grid_fits(weights, cotangents, tokens, rank):
    rows = weights[0].shape[0]
    tokens_here, owned = tokens.shape
    count = tokens_here // token_lanes
    aligned = all(c.shape[1] % token_lanes == 0 for c in cotangents) and owned % token_lanes == 0
    return (
        aligned and rows % 32 == 0 and tokens_here % token_lanes == 0
        and count in (3, 4) and rank == 16 and owned == 8 * rows
    )


def grid_step(tokens, gain, weights, adapters, ups, cotangents):
    rows = weights[0].shape[0]
    tokens_here, owned = tokens.shape
    full_width = gain.shape[0]
    rank = adapters.shape[1]
    depth = sum(w.shape[1] for w in weights)
    half = rows // 2
    lanes = token_lanes
    count = tokens_here // lanes
    number = len(piece_rows(half))
    scale = adapter_scale / math.sqrt(tokens_here * lax.axis_size("fsdp"))
    grad_blocks = 16 * -(-(3 * owned + depth) // (16 * lanes))
    share = grad_blocks // 2
    DMA = pltpu.SemaphoreType.DMA
    f32, bf16 = jnp.float32, jnp.bfloat16
    vmem = pl.BlockSpec(memory_space=pltpu.VMEM)
    return pl.pallas_call(
        functools.partial(grid_kernel, (full_width, owned, rank, scale)),
        out_shape=(
            jax.ShapeDtypeStruct(tokens.shape, bf16),
            jax.ShapeDtypeStruct((3, rank, owned), f32),
        ) + tuple(jax.ShapeDtypeStruct((rank, c.shape[1]), f32) for c in cotangents),
        in_specs=[pl.BlockSpec(memory_space=pl.ANY)] * 12,
        out_specs=(vmem,) * 5,
        scratch_shapes=[
            pltpu.VMEM((8, half, depth), bf16),
            pltpu.VMEM((2 * count, 2 * lanes, depth), bf16),
            pltpu.VMEM((8, 2 * count, 2, half, lanes), bf16),
            pltpu.VMEM((4, 2 * count, 2, half, lanes), bf16),
            pltpu.VMEM((count, 8 * rows, lanes), bf16),
            pltpu.VMEM((tokens_here, owned), bf16),
            pltpu.VMEM((1, owned), f32),
            pltpu.VMEM((lanes, depth), bf16),
            pltpu.VMEM((lanes, owned), bf16),
            pltpu.VMEM((3, lanes, owned), bf16),
            pltpu.VMEM((count, lanes, lanes), f32),
            pltpu.VMEM((count, lanes, lanes), f32),
            pltpu.VMEM((count, lanes, lanes), f32),
            pltpu.VMEM((count, lanes, lanes), bf16),
            pltpu.VMEM((lanes, tokens_here), bf16),
            pltpu.VMEM((tokens_here, owned), bf16),
            pltpu.VMEM((tokens_here, owned), f32),
            pltpu.VMEM((count, lanes, lanes), f32),
            pltpu.VMEM((count, lanes, lanes), f32),
            pltpu.VMEM((grad_blocks, rank, lanes), f32),
            pltpu.VMEM((share, rank, lanes), f32),
            pltpu.VMEM((share // 2, rank, lanes), f32),
            pltpu.VMEM((share // 2, rank, lanes), bf16),
            pltpu.VMEM((3, share // 8, rank, lanes), bf16),
            pltpu.VMEM((grad_blocks, rank, lanes), bf16),
            DMA((2, 3)), DMA((count, 3)), DMA((8,)),
            DMA, DMA, DMA, DMA((count,)),
            DMA, DMA, DMA, DMA, DMA, DMA((3,)), DMA, DMA((3,)), DMA, DMA, DMA, DMA,
            DMA, DMA((count,)), DMA, DMA((count,)), DMA, DMA((count,)),
            DMA, DMA((2,)), DMA, DMA((2, number)), DMA, DMA((2, number)),
            DMA, DMA((4, 2 * count)), DMA, DMA,
        ],
        compiler_params=pltpu.CompilerParams(
            collective_id=0, has_side_effects=True, vmem_limit_bytes=60 * 1024 * 1024
        ),
        cost_estimate=pl.CostEstimate(
            flops=2 * 16 * rows * tokens_here * depth, bytes_accessed=2 * 8 * rows * depth,
            transcendentals=0,
        ),
        name="grid",
    )(*cotangents, *weights, tokens, gain.reshape(1, full_width), adapters, *ups)


def shards(
    tokens,
    gain,
    query_projection_weight,
    key_projection_weight,
    value_projection_weight,
    adapter_down_factors,
    query_adapter_up,
    key_adapter_up,
    value_adapter_up,
    query_cotangent,
    key_cotangent,
    value_cotangent,
):
    return device_work(
        tokens,
        gain,
        (query_projection_weight, key_projection_weight, value_projection_weight),
        adapter_down_factors,
        (query_adapter_up, key_adapter_up, value_adapter_up),
        (query_cotangent, key_cotangent, value_cotangent),
    )


def device_work(tokens, gain, weights, adapter_down_factors, ups, cots):
    fsdp_size = lax.axis_size("fsdp")
    tp_size = lax.axis_size("tp")
    tp_index = lax.axis_index("tp")
    row_count, owned = tokens.shape
    full_width = gain.shape[0]
    rank = adapter_down_factors.shape[1]
    if tp_size == 2 and fsdp_size == 16 and grid_fits(weights, cots, tokens, rank):
        return grid_step(tokens, gain, weights, adapter_down_factors, ups, cots)

    def tp_sum(value):
        if tp_size != 2:
            return lax.psum(value, "tp")
        with jax.named_scope("pair_sum"):
            return value + lax.ppermute(value, "tp", [(0, 1), (1, 0)])

    wide = tokens.astype(jnp.float32)
    gain_own = lax.dynamic_slice_in_dim(gain, tp_index * owned, owned, 0)
    down = lax.dynamic_slice_in_dim(adapter_down_factors, tp_index * owned, owned, 2)
    down = down.reshape(3 * rank, owned)
    low_in = lax.dot_general(
        wide * gain_own[None, :],
        down.astype(jnp.float32),
        (((1,), (1,)), ((), ())),
        precision=lax.Precision.HIGHEST,
    )
    low_out = jnp.concatenate([transposed_product(c, u) for c, u in zip(cots, ups)], axis=1)
    squares = jnp.sum(wide * wide, axis=1, keepdims=True)
    small = tp_sum(jnp.concatenate([squares, low_in, low_out], axis=1))
    inverse = lax.rsqrt(small[:, :1] / full_width + norm_eps)
    in_low = (small[:, 1 : 1 + 3 * rank] * inverse).astype(jnp.bfloat16)
    out_low = small[:, 1 + 3 * rank :].astype(jnp.bfloat16)
    unit_rows = wide * inverse
    normed = (unit_rows * gain_own[None, :]).astype(jnp.bfloat16)
    scale = adapter_scale / math.sqrt(row_count * fsdp_size)

    def token_product(left, right):
        return scale * lax.dot_general(
            left, right, (((0,), (0,)), ((), ())), preferred_element_type=jnp.float32
        )

    down_local = token_product(out_low, normed)
    up_local = [
        token_product(in_low[:, rank * m : rank * (m + 1)], cots[m]) for m in range(3)
    ]
    small_work = tuple(down_local[rank * m : rank * (m + 1)] for m in range(3)) + tuple(up_local)
    back = plain_back(weights, cots, full_width)
    grads = lax.psum(jnp.concatenate(small_work, axis=1), "fsdp")
    grad_down = jnp.stack([grads[:, owned * m : owned * (m + 1)] for m in range(3)])
    ends = [3 * owned]
    for cot in cots:
        ends.append(ends[-1] + cot.shape[1])
    up_q, up_k, up_v = [grads[:, low:high] for low, high in zip(ends[:-1], ends[1:])]

    back = back + adapter_scale * jnp.dot(out_low, down, preferred_element_type=jnp.float32)
    gained = gain_own[None, :] * back
    inner = tp_sum(jnp.sum(gained * unit_rows, axis=1, keepdims=True)) / full_width
    grad_tokens = (inverse * (gained - unit_rows * inner)).astype(jnp.bfloat16)
    return (grad_tokens, grad_down, up_q, up_k, up_v)


def solution(mesh):
    in_specs = (
        P("fsdp", "tp"),
        P(),
        P("fsdp", "tp"),
        P("fsdp", "tp"),
        P("fsdp", "tp"),
        P(),
        P(None, "tp"),
        P(None, "tp"),
        P(None, "tp"),
        P("fsdp", "tp"),
        P("fsdp", "tp"),
        P("fsdp", "tp"),
    )
    out_specs = (P("fsdp", "tp"), P(None, None, "tp"), P(None, "tp"), P(None, "tp"), P(None, "tp"))
    step = jax.shard_map(shards, mesh=mesh, in_specs=in_specs, out_specs=out_specs, check_vma=False)
    return step
```

```python
import functools
import math

import jax
import jax.numpy as jnp
from jax import lax
from jax.experimental import pallas as pl
from jax.experimental.pallas import tpu as pltpu
from jax.sharding import PartitionSpec as P

norm_eps = 1e-05
adapter_scale = 2.0


def transposed_product(left, right):
    return lax.dot_general(
        left, right, (((1,), (1,)), ((), ())), preferred_element_type=jnp.float32
    )


def plain_back(weights, cotangents, full_width):
    total = jnp.zeros((cotangents[0].shape[0], full_width), jnp.float32)
    for weight, cotangent in zip(weights, cotangents):
        whole = lax.all_gather(weight, "fsdp", axis=0, tiled=True)
        total = total + transposed_product(cotangent, whole)
    return lax.psum_scatter(total, "tp", scatter_dimension=1, tiled=True)


def near_and_far_orders(count):
    near = list(range(count))
    every = list(range(2 * count))
    outer, outer_marks = [], {}
    inner, inner_marks = [], {}

    def add(order, marks, name, groups, ts):
        marks[name] = len(order)
        order.extend((w, t, n) for t in ts for w, n in groups)

    own, row = (0, 2), (2, 2)
    first, second = (4, 2), (6, 2)
    add(outer, outer_marks, "near", [own], near)
    add(outer, outer_marks, "f0", [(4, 1)], near)
    add(outer, outer_marks, "y", [row], near)
    add(outer, outer_marks, "f1", [(6, 1)], near)
    late = [(4, 1), (6, 1)]
    for i in range(count):
        add(outer, outer_marks, f"z{i}", [own, row] + late, [count + i])
        if i == count - 3:
            add(outer, outer_marks, "fy0", [(5, 1)], range(count + i + 1))
            late = [first, (6, 1)]
        if i == count - 2:
            add(outer, outer_marks, "fy1", [(7, 1)], range(count + i + 1))
            late = [first, second]
    add(inner, inner_marks, "near", [own], near)
    for i in range(count):
        add(inner, inner_marks, f"z{i}", [own], [count + i])
    add(inner, inner_marks, "y", [row], every)
    add(inner, inner_marks, "f0", [(4, 1)], every)
    add(inner, inner_marks, "fy0", [(5, 1)], every)
    add(inner, inner_marks, "f1", [(6, 1)], every)
    add(inner, inner_marks, "fy1", [(7, 1)], every)
    steps = max(len(outer), len(inner))
    lengths = len(outer), len(inner)
    for order in (outer, inner):
        order.extend([(0, 0, 0)] * (steps - len(order)))
    return (outer, outer_marks), (inner, inner_marks), lengths


def packed(digits):
    words = []
    for low in range(0, len(digits), 10):
        words.append(sum(d << (3 * k) for k, d in enumerate(digits[low : low + 10])))
    return words


def digit_at(step, is_inner, outer_digits, inner_digits):
    word = jnp.int32(0)
    for k, (o, i) in enumerate(zip(packed(outer_digits), packed(inner_digits))):
        value = jnp.where(is_inner == 1, jnp.int32(i), jnp.int32(o))
        word = jnp.where(step // 10 == k, value, word)
    return lax.shift_right_logical(word, 3 * (step % 10)) % 8


def piece_rows(half):
    size = 48 if half > 48 else half
    cuts = list(range(0, half, size)) + [half]
    return list(zip(cuts[:-1], cuts[1:]))


def grid_kernel(
    settings,
    cq, ck, cv, wq, wk, wv, tokens, gain, adapters, uq, uk, uv,
    out, inner_out, inverse_out, grad_down, grad_up_q, grad_up_k, grad_up_v,
    W, C, S, X, R,
    T, GW, GA, U, D, GD, A, AR, INV, LO, ZT, N, B, I, IR,
    G, GC, GY, H, HZ, F,
    load_w, load_c, load_s, store_sem,
    a_send, a_recv, i_send, i_recv,
    gc_send, gc_recv, gy_send, gy_recv, gz_send, gz_recv, ga_send, ga_recv, gb_send, gb_recv, gd_send, gd_recv,
    cc_send, cc_recv, cz_send, cz_recv, zc_send, zc_recv,
    y_send, y_recv, far_send, far_recv, fy_send, fy_recv,
    x_send, x_recv, r_send, r_recv,
):
    half = W.shape[1]
    block = 2 * half
    count = C.shape[0] // 2
    lanes = R.shape[2]
    top = 8
    place = lax.axis_index("fsdp")
    side = lax.axis_index("tp")

    def flipped(bit):
        return place + bit * (1 - 2 * ((place // bit) % 2))

    def at(bit):
        return {"fsdp": flipped(bit), "tp": side}

    def both(one, two):
        return {"fsdp": flipped(one) + flipped(two) - place, "tp": side}

    core, row, near_z, far_z = at(1), at(2), at(4), at(8)
    diagonal, third_z = both(4, 1), both(4, 8)
    twin = {"fsdp": place, "tp": 1 - side}
    z = place // 4
    is_inner = ((z + 1) // 2) % 2
    keep_late = (place // top + side) % 2

    pieces = piece_rows(half)
    columns = []
    low = 0
    for ref in (cq, ck, cv):
        columns.append((low, low + ref.shape[1]))
        low += ref.shape[1]

    def load_cot(i, m):
        low, high = columns[m]
        ref = (cq, ck, cv)[m]
        return pltpu.make_async_copy(
            ref.at[pl.ds(i * lanes, lanes), :],
            C.at[i, pl.ds(0, lanes), pl.ds(low, high - low)],
            load_c.at[i, m],
        )

    def load_weight(h, m):
        low, high = columns[m]
        ref = (wq, wk, wv)[m]
        return pltpu.make_async_copy(
            ref.at[pl.ds(h * half, half), :],
            W.at[h, :, pl.ds(low, high - low)],
            load_w.at[h, m],
        )

    def remote(src, dst, send, recv, device):
        return pltpu.make_async_remote_copy(
            src_ref=src, dst_ref=dst, send_sem=send, recv_sem=recv,
            device_id=device, device_id_type=pl.DeviceIdType.MESH,
        )

    lower, upper = pl.ds(0, lanes), pl.ds(lanes, lanes)
    full_width, owned, rank, scale = settings
    own_columns = pl.ds(pl.multiple_of(side * owned, lanes), owned)
    feature_blocks = owned // lanes
    share = F.shape[0] // 2
    core_index, row_index = place % 2, (place // 2) % 2
    part_start = core_index * share + row_index * (share // 2)
    piece = share // 8

    small_loads = [
        pltpu.make_async_copy(tokens, T, load_s.at[0]),
        pltpu.make_async_copy(gain, GW, load_s.at[1]),
    ]
    for m in range(3):
        small_loads.append(
            pltpu.make_async_copy(
                adapters.at[m, :, own_columns], D.at[pl.ds(rank * m, rank)], load_s.at[2 + m]
            )
        )
        low, high = columns[m]
        small_loads.append(
            pltpu.make_async_copy(
                (uq, uk, uv)[m],
                U.at[pl.ds(rank * m, rank), pl.ds(low, high - low)],
                load_s.at[5 + m],
            )
        )

    def pair_rows():
        return remote(A, AR, a_send, a_recv, twin)

    def inner_rows(i):
        return remote(I.at[i], IR.at[i], i_send, i_recv.at[i], twin)

    def grads_core():
        away = (1 - core_index) * share
        return remote(G.at[pl.ds(away, share)], GC, gc_send, gc_recv, core)

    def grads_row():
        away = core_index * share + (1 - row_index) * (share // 2)
        return remote(G.at[pl.ds(away, share // 2)], GY, gy_send, gy_recv, row)

    z_partners = ((near_z, 1), (far_z, 2), (third_z, 3))

    def z_flip(bits):
        low, high = z % 2, z // 2
        low = 1 - low if bits % 2 else low
        high = 1 - high if bits // 2 else high
        return 2 * high + low

    def grads_z(n):
        device, bits = z_partners[n]
        return remote(
            H.at[pl.ds(z_flip(bits) * piece, piece)], HZ.at[n], gz_send, gz_recv.at[n], device
        )

    mine_z = pl.ds(part_start + z * piece, piece)
    mine_y = pl.ds(part_start, share // 2)
    mine_c = pl.ds(core_index * share, share)

    def spread_z(n):
        return remote(F.at[mine_z], F.at[mine_z], ga_send, ga_recv.at[n], z_partners[n][0])

    def spread_y():
        return remote(F.at[mine_y], F.at[mine_y], gb_send, gb_recv, row)

    def spread_c():
        return remote(F.at[mine_c], F.at[mine_c], gd_send, gd_recv, core)

    def cot_core(i):
        return remote(C.at[i, lower], C.at[i, upper], cc_send, cc_recv.at[i], core)

    def cot_z(i):
        return remote(C.at[i, lower], C.at[count + i, lower], cz_send, cz_recv.at[i], near_z)

    cot_pieces = [(i, low) for i in range(count) for low in range(0, lanes, 32)]

    def start_cot_pieces(low, high):
        for i, first in cot_pieces[low:high]:
            rows = pl.ds(first, 32)
            remote(
                C.at[i, rows], C.at[count + i, rows], cz_send, cz_recv.at[i], near_z
            ).start()

    def cot_zc(i):
        return remote(
            C.at[count + i, lower], C.at[count + i, upper], zc_send, zc_recv.at[i], core
        )

    def weight_y(h):
        return remote(W.at[h], W.at[2 + h], y_send, y_recv.at[h], row)

    def far(h, k):
        low, high = pieces[k]
        rows = pl.ds(low, high - low)
        return remote(W.at[h, rows], W.at[4 + 2 * h, rows], far_send, far_recv.at[h, k], far_z)

    def far_y(h, k):
        low, high = pieces[k]
        rows = pl.ds(low, high - low)
        return remote(W.at[4 + 2 * h, rows], W.at[5 + 2 * h, rows], fy_send, fy_recv.at[h, k], row)

    for i in range(count):
        for m in range(3):
            load_cot(i, m).start()
    for h in range(2):
        for m in range(3):
            load_weight(h, m).start()
    for copy in small_loads:
        copy.start()

    barrier = pltpu.get_barrier_semaphore()
    partners = (core, row, near_z, diagonal, far_z, third_z, twin)
    for partner in partners:
        pl.semaphore_signal(
            barrier, inc=1, device_id=partner, device_id_type=pl.DeviceIdType.MESH
        )
    pl.semaphore_wait(barrier, len(partners))

    for i in range(count):
        for m in range(3):
            load_cot(i, m).wait()

        @pl.when(is_inner == 0)
        def _():
            cot_z(i).start()

    for h in range(2):
        for m in range(3):
            load_weight(h, m).wait()

        @pl.when(is_inner == 1)
        def _():
            for k in range(len(pieces)):
                far(h, k).start()

        if h == 0:
            weight_y(h).start()
    for i in range(count):
        cot_core(i).start()

    lane = lax.broadcasted_iota(jnp.int32, (lanes, lanes), 1)
    used = 3 * rank
    D[pl.ds(used, lanes - used), :] = jnp.zeros((lanes - used, owned), jnp.bfloat16)
    U[pl.ds(used, lanes - used), :] = jnp.zeros((lanes - used, U.shape[1]), jnp.bfloat16)
    for m in range(3):
        for other in range(3):
            if other != m:
                low, high = columns[other]
                U[pl.ds(rank * m, rank), pl.ds(low, high - low)] = jnp.zeros(
                    (rank, high - low), jnp.bfloat16
                )
    for p in range(3):
        GD[p] = jnp.zeros((lanes, owned), jnp.bfloat16)
    for copy in small_loads:
        copy.wait()
    for j in range(feature_blocks):
        GA[:, pl.ds(j * lanes, lanes)] = GW[pl.ds(side * feature_blocks + j, 1), :]
    rest = D[pl.ds(0, used), :].astype(jnp.float32) * GA[...]
    for p in range(3):
        part = rest.astype(jnp.bfloat16)
        GD[p, pl.ds(64, used), :] = part
        rest = rest - part.astype(jnp.float32)

    def nt_dot(left, right):
        return lax.dot_general(
            left, right, (((1,), (1,)), ((), ())), preferred_element_type=jnp.float32
        )

    for i in range(count):
        rows = pl.ds(i * lanes, lanes)
        own_rows = T[rows, :]
        value = nt_dot(C[i, lower, :], U[...])
        for p in range(3):
            value = value + nt_dot(own_rows, GD[p])
        wide = own_rows.astype(jnp.float32)
        squares = jnp.sum(wide * wide, axis=1, keepdims=True)
        A[i] = value + jnp.where(lane == 120, squares, 0.0)
    pair_rows().start()
    pair_rows().wait_recv()
    for i in range(count):
        rows = pl.ds(i * lanes, lanes)
        both_sum = A[i] + AR[i]
        squares = jnp.sum(jnp.where(lane == 120, both_sum, 0.0), axis=1, keepdims=True)
        inverse = lax.rsqrt(squares / full_width + norm_eps)
        INV[i] = jnp.broadcast_to(inverse, (lanes, lanes))
        low = jnp.where(lane < used, both_sum, 0.0)
        LO[i] = low.astype(jnp.bfloat16)
        scaled = jnp.where((lane >= 64) & (lane < 64 + used), both_sum * inverse, 0.0)
        ZT[:, rows] = (low + scaled).T.astype(jnp.bfloat16)
        N[rows, :] = (T[rows, :].astype(jnp.float32) * inverse * GA[...]).astype(jnp.bfloat16)

    def down_block(j, carry):
        cols = pl.ds(pl.multiple_of(j * lanes, lanes), lanes)
        value = scale * jnp.dot(
            ZT[pl.ds(0, 64), :], N[:, cols], preferred_element_type=jnp.float32
        )
        for m in range(3):
            G[m * feature_blocks + j] = value[rank * m : rank * (m + 1)]
        return carry

    lax.fori_loop(0, feature_blocks, down_block, 0)
    first = 3 * feature_blocks
    for m in range(3):
        low, high = columns[m]

        def up_block(j, carry, m=m, low=low):
            cols = pl.ds(pl.multiple_of(low + j * lanes, lanes), lanes)
            value = jnp.zeros((rank, lanes), jnp.float32)
            for i in range(count):
                value = value + jnp.dot(
                    ZT[pl.ds(64 + rank * m, rank), pl.ds(i * lanes, lanes)],
                    C[i, lower, cols],
                    preferred_element_type=jnp.float32,
                )
            G[first + low // lanes + j] = scale * value
            return carry

        lax.fori_loop(0, (high - low) // lanes, up_block, 0)
    filled = first + columns[2][1] // lanes
    for j in range(filled, G.shape[0]):
        G[j] = jnp.zeros((rank, lanes), jnp.float32)
    grads_core().start()
    grads_core().wait_recv()
    G[mine_c] = G[mine_c] + GC[...]
    grads_row().start()
    weight_y(1).start()

    (outer, outer_marks), (inner, inner_marks), lengths = near_and_far_orders(count)
    tiles = is_inner * lengths[1] + (1 - is_inner) * lengths[0]
    lag = 3

    def order_at(step):
        return [
            digit_at(step, is_inner, [a[k] for a in outer], [a[k] for a in inner])
            for k in range(3)
        ]

    def when(step, outer_name, inner_name, inner_shift=0):
        o = outer_marks[outer_name] if outer_name else -1
        i = inner_marks[inner_name] + inner_shift if inner_name else -1
        return pl.when(step == is_inner * i + (1 - is_inner) * o)

    def take_far(h, k):
        far(h, k).wait_recv()
        far_y(h, k).start()

    last_outer = f"z{count - 1}"
    last_step = is_inner * inner_marks["f1"] + (1 - is_inner) * outer_marks[last_outer]
    waiting = is_inner * count + (1 - is_inner) * (count - 1)

    def sum_rows(slot):
        base = place % top
        other = keep_late * (slot % 2) + (1 - keep_late) * (slot // 2)
        part = keep_late * (slot // 2) + (1 - keep_late) * (slot % 2)
        index = base + other * 2 * (1 - 2 * ((base // 2) % 2))
        return pl.ds(pl.multiple_of(index * block + part * half, 16), half)

    def return_far(mine, t2, rows):
        i = t2 - count
        remote(S.at[mine, t2, 0], R.at[i, rows], r_send, r_recv.at[i], near_z).start()
        remote(S.at[mine, t2, 1], R.at[i, rows], r_send, r_recv.at[i], diagonal).start()

    def return_held(n, carry):
        slot, i = n % 4, n // 4
        return_far(slot, count + i, sum_rows(slot))
        return carry

    def body(step, carry):
        @when(step, "near", "near")
        def _():
            for i in range(count):
                cot_core(i).wait_recv()

        @when(step, None, f"z{count - 1}")
        def _():
            remote(W.at[pl.ds(0, 2)], W.at[pl.ds(4, 2)], far_send, far_recv.at[0, 0], far_z).wait_send()
            start_cot_pieces(0, 4)

        @when(step, "f0", "z1")
        def _():
            grads_row().wait_recv()
            G[mine_y] = G[mine_y] + GY[...]
            H[...] = G[mine_y].astype(jnp.bfloat16)
            for n in range(3):
                grads_z(n).start()

        @when(step, "y", None)
        def _():
            for k in range(len(pieces)):
                far(0, k).start()

        @when(step, "z0", "f0")
        def _():
            value = G[mine_z]
            for n in range(3):
                grads_z(n).wait_recv()
                value = value + HZ[n].astype(jnp.float32)
            F[mine_z] = value.astype(jnp.bfloat16)
            for n in range(3):
                spread_z(n).start()

        @when(step, "z0", None)
        def _():
            for k in range(len(pieces)):
                far(1, k).start()

        @when(step, last_outer, "fy1")
        def _():
            for n in range(3):
                spread_z(n).wait_recv()
            spread_y().start()

        for i in range(count):
            @when(step, f"z{i}", f"z{i}")
            def _():
                cot_z(i).wait_recv()
                cot_zc(i).start()
                cot_zc(i).wait_recv()

        @when(step, "y", "y")
        def _():
            weight_y(0).wait_recv()
            weight_y(1).wait_recv()

        number = len(pieces)

        @when(step, "f0", None)
        def _():
            for k in range(number):
                take_far(0, k)

        @when(step, "f1", None)
        def _():
            for k in range(number):
                take_far(1, k)

        @pl.when((step == last_step) & (keep_late == 0))
        def _():
            lax.fori_loop(0, 4 * waiting, return_held, 0)

        waves = number // 2
        extra = -(-(len(cot_pieces) - 4) // number)
        takes = [("f0", (k - number + 2) * 3 if k < number - 2 else 0) for k in range(number)]
        takes += [("fy0", 0)] * waves + [("f1", 0)] * (number - waves)
        for k, (name, shift) in enumerate(takes):
            @when(step, None, name, shift)
            def _():
                take_far(k // number, k % number)
                if k < number:
                    start_cot_pieces(4 + extra * k, 4 + extra * (k + 1))

        for h in range(2):
            @when(step, f"fy{h}", f"fy{h}")
            def _():
                for k in range(number):
                    far_y(h, k).wait_recv()

        w, t, n = order_at(step)

        def product(size):
            value = lax.dot_general(
                W[pl.ds(w, size)].reshape(size * half, W.shape[2]),
                C[t],
                (((1,), (1,)), ((), ())),
                preferred_element_type=jnp.float32,
            ).astype(jnp.bfloat16)
            for q in range(size):
                for part in range(2):
                    S[w + q, t, part] = value[
                        half * q : half * (q + 1), lanes * part : lanes * (part + 1)
                    ]

        @pl.when((step < tiles) & (n == 1))
        def _():
            product(1)

        @pl.when((step < tiles) & (n == 2))
        def _():
            product(2)

        for q in range(2):
            @pl.when((step < tiles) & (q < n) & (w // 4 != keep_late))
            def _():
                remote(
                    S.at[w + q, t], X.at[w % 4 + q, t], x_send, x_recv.at[w % 4 + q, t], twin
                ).start()

        back = jnp.maximum(step - lag, 0)
        w2, t2, n2 = order_at(back)

        for q in range(2):
            @pl.when((step >= lag) & (step < tiles + lag) & (q < n2) & (w2 // 4 == keep_late))
            def _():
                mine, slot = w2 + q, w2 % 4 + q
                remote(
                    S.at[mine, t2], X.at[slot, t2], x_send, x_recv.at[slot, t2], twin
                ).wait_recv()
                total = S[mine, t2].astype(jnp.float32) + X[slot, t2].astype(jnp.float32)
                S[mine, t2] = total.astype(jnp.bfloat16)
                rows = sum_rows(slot)
                i = t2 % count

                @pl.when(t2 < count)
                def _():
                    R[i, rows, :] = total[0].astype(jnp.bfloat16)
                    remote(S.at[mine, t2, 1], R.at[i, rows], r_send, r_recv.at[i], core).start()

                @pl.when((t2 >= count) & ((keep_late == 1) | (t2 >= count + waiting)))
                def _():
                    return_far(mine, t2, rows)

        return carry

    lax.fori_loop(0, max(lengths) + lag, body, 0)

    spread_y().wait_recv()
    spread_c().start()
    spread_c().wait_recv()
    for j in range(feature_blocks):
        for m in range(3):
            grad_down[m, :, pl.ds(j * lanes, lanes)] = F[m * feature_blocks + j].astype(jnp.float32)
    for m, ref in enumerate((grad_up_q, grad_up_k, grad_up_v)):
        low, high = columns[m]
        for j in range((high - low) // lanes):
            ref[:, pl.ds(j * lanes, lanes)] = F[first + low // lanes + j].astype(jnp.float32)
    part = pl.ds(0, 3 * R.shape[1] // 4)
    stores = []
    for i in range(count):
        rows = pl.ds(i * lanes, lanes)
        remote(R.at[i, part], R.at[i, part], r_send, r_recv.at[i], core).wait_recv()
        inverse = INV[i]

        def gained_block(j, carry, i=i, rows=rows, inverse=inverse):
            cols = pl.ds(pl.multiple_of(j * lanes, lanes), lanes)
            back = R[i, cols, :].astype(jnp.float32).T
            back = back + adapter_scale * jnp.dot(
                LO[i], D[:, cols], preferred_element_type=jnp.float32
            )
            gained = GA[:, cols] * back
            B[rows, cols] = gained
            return carry + gained * (T[rows, cols].astype(jnp.float32) * inverse)

        total = lax.fori_loop(
            0, feature_blocks, gained_block, jnp.zeros((lanes, lanes), jnp.float32), unroll=2
        )
        I[i] = jnp.broadcast_to(jnp.sum(total, axis=1, keepdims=True), (lanes, lanes))
        inner_rows(i).start()
        stores.append(pltpu.make_async_copy(B.at[rows], out.at[rows], store_sem.at[i]))
        stores[-1].start()
    for i in range(count):
        rows = pl.ds(i * lanes, lanes)
        inner_rows(i).wait_recv()
        inner_out[rows, :] = (I[i] + IR[i]) / full_width
        inverse_out[rows, :] = INV[i]

    results = remote(R.at[:, part], R.at[:, part], r_send, r_recv.at[0], core)
    results.wait_send()
    own = C.at[pl.ds(0, count), lower]
    remote(own, own, cc_send, cc_recv.at[0], core).wait_send()
    remote(own, own, cz_send, cz_recv.at[0], core).wait_send()
    remote(own, own, zc_send, zc_recv.at[0], core).wait_send()
    two = W.at[pl.ds(0, 2)]
    remote(two, two, y_send, y_recv.at[0], core).wait_send()

    @pl.when(is_inner == 0)
    def _():
        remote(two, two, far_send, far_recv.at[0, 0], core).wait_send()

    remote(two, two, fy_send, fy_recv.at[0, 0], core).wait_send()
    four = S.at[pl.ds(0, 4)]
    remote(four, four, x_send, x_recv.at[0, 0], core).wait_send()
    pair_rows().wait_send()
    remote(I, I, i_send, i_recv.at[0], twin).wait_send()
    grads_core().wait_send()
    grads_row().wait_send()
    three = H.at[pl.ds(0, 3 * piece)]
    remote(three, three, gz_send, gz_recv.at[0], core).wait_send()
    three = F.at[pl.ds(0, 3 * piece)]
    remote(three, three, ga_send, ga_recv.at[0], core).wait_send()
    spread_y().wait_send()
    spread_c().wait_send()
    for store in stores:
        store.wait()


token_lanes = 128


def final_kernel(gained, tokens, inner, inverse, *refs):
    grads, (out, *grad_outs) = refs[:4], refs[4:]

    @pl.when(pl.program_id(0) == 0)
    def _():
        for source, target in zip(grads, grad_outs):
            target[...] = source[...]

    scale = inverse[:, :1]
    unit = tokens[...].astype(jnp.float32) * scale
    out[...] = (scale * (gained[...] - unit * inner[:, :1])).astype(out.dtype)


def grid_fits(weights, cotangents, tokens, rank):
    rows = weights[0].shape[0]
    tokens_here, owned = tokens.shape
    count = tokens_here // token_lanes
    aligned = all(c.shape[1] % token_lanes == 0 for c in cotangents) and owned % token_lanes == 0
    return (
        aligned and rows % 32 == 0 and tokens_here % token_lanes == 0
        and count in (3, 4) and rank == 16 and owned == 8 * rows
    )


def grid_step(tokens, gain, weights, adapters, ups, cotangents):
    rows = weights[0].shape[0]
    tokens_here, owned = tokens.shape
    full_width = gain.shape[0]
    rank = adapters.shape[1]
    depth = sum(w.shape[1] for w in weights)
    half = rows // 2
    lanes = token_lanes
    count = tokens_here // lanes
    number = len(piece_rows(half))
    scale = adapter_scale / math.sqrt(tokens_here * lax.axis_size("fsdp"))
    grad_blocks = 16 * -(-(3 * owned + depth) // (16 * lanes))
    share = grad_blocks // 2
    DMA = pltpu.SemaphoreType.DMA
    f32, bf16 = jnp.float32, jnp.bfloat16
    vmem = pl.BlockSpec(memory_space=pltpu.VMEM)
    gained, inner, inverse, *grads = pl.pallas_call(
        functools.partial(grid_kernel, (full_width, owned, rank, scale)),
        out_shape=(
            jax.ShapeDtypeStruct(tokens.shape, f32),
            jax.ShapeDtypeStruct((tokens_here, lanes), f32),
            jax.ShapeDtypeStruct((tokens_here, lanes), f32),
            jax.ShapeDtypeStruct((3, rank, owned), f32),
        ) + tuple(jax.ShapeDtypeStruct((rank, c.shape[1]), f32) for c in cotangents),
        in_specs=[pl.BlockSpec(memory_space=pl.ANY)] * 12,
        out_specs=(pl.BlockSpec(memory_space=pl.ANY),) + (vmem,) * 6,
        scratch_shapes=[
            pltpu.VMEM((8, half, depth), bf16),
            pltpu.VMEM((2 * count, 2 * lanes, depth), bf16),
            pltpu.VMEM((8, 2 * count, 2, half, lanes), bf16),
            pltpu.VMEM((4, 2 * count, 2, half, lanes), bf16),
            pltpu.VMEM((count, 8 * rows, lanes), bf16),
            pltpu.VMEM((tokens_here, owned), bf16),
            pltpu.VMEM((full_width // lanes, lanes), f32),
            pltpu.VMEM((1, owned), f32),
            pltpu.VMEM((lanes, depth), bf16),
            pltpu.VMEM((lanes, owned), bf16),
            pltpu.VMEM((3, lanes, owned), bf16),
            pltpu.VMEM((count, lanes, lanes), f32),
            pltpu.VMEM((count, lanes, lanes), f32),
            pltpu.VMEM((count, lanes, lanes), f32),
            pltpu.VMEM((count, lanes, lanes), bf16),
            pltpu.VMEM((lanes, tokens_here), bf16),
            pltpu.VMEM((tokens_here, owned), bf16),
            pltpu.VMEM((tokens_here, owned), f32),
            pltpu.VMEM((count, lanes, lanes), f32),
            pltpu.VMEM((count, lanes, lanes), f32),
            pltpu.VMEM((grad_blocks, rank, lanes), f32),
            pltpu.VMEM((share, rank, lanes), f32),
            pltpu.VMEM((share // 2, rank, lanes), f32),
            pltpu.VMEM((share // 2, rank, lanes), bf16),
            pltpu.VMEM((3, share // 8, rank, lanes), bf16),
            pltpu.VMEM((grad_blocks, rank, lanes), bf16),
            DMA((2, 3)), DMA((count, 3)), DMA((8,)), DMA((count,)),
            DMA, DMA, DMA, DMA((count,)),
            DMA, DMA, DMA, DMA, DMA, DMA((3,)), DMA, DMA((3,)), DMA, DMA, DMA, DMA,
            DMA, DMA((count,)), DMA, DMA((count,)), DMA, DMA((count,)),
            DMA, DMA((2,)), DMA, DMA((2, number)), DMA, DMA((2, number)),
            DMA, DMA((4, 2 * count)), DMA, DMA((count,)),
        ],
        compiler_params=pltpu.CompilerParams(
            collective_id=0, has_side_effects=True, vmem_limit_bytes=60 * 1024 * 1024
        ),
        cost_estimate=pl.CostEstimate(
            flops=2 * 16 * rows * tokens_here * depth, bytes_accessed=2 * 8 * rows * depth,
            transcendentals=0,
        ),
        name="grid",
    )(*cotangents, *weights, tokens, gain.reshape(full_width // lanes, lanes), adapters, *ups)
    step_rows = 64

    def by_rows(width):
        return pl.BlockSpec((step_rows, width), lambda i: (i, 0))

    whole = [pl.BlockSpec(g.shape, lambda i, k=len(g.shape): (0,) * k) for g in grads]
    return pl.pallas_call(
        final_kernel,
        grid=(tokens_here // step_rows,),
        out_shape=(jax.ShapeDtypeStruct(tokens.shape, bf16),)
        + tuple(jax.ShapeDtypeStruct(g.shape, f32) for g in grads),
        in_specs=[by_rows(owned), by_rows(owned), by_rows(lanes), by_rows(lanes), *whole],
        out_specs=(by_rows(owned), *whole),
        cost_estimate=pl.CostEstimate(
            flops=4 * tokens_here * owned, bytes_accessed=8 * tokens_here * owned, transcendentals=0
        ),
        name="final",
    )(gained, tokens, inner, inverse, *grads)


def shards(
    tokens,
    gain,
    query_projection_weight,
    key_projection_weight,
    value_projection_weight,
    adapter_down_factors,
    query_adapter_up,
    key_adapter_up,
    value_adapter_up,
    query_cotangent,
    key_cotangent,
    value_cotangent,
):
    return device_work(
        tokens,
        gain,
        (query_projection_weight, key_projection_weight, value_projection_weight),
        adapter_down_factors,
        (query_adapter_up, key_adapter_up, value_adapter_up),
        (query_cotangent, key_cotangent, value_cotangent),
    )


def device_work(tokens, gain, weights, adapter_down_factors, ups, cots):
    fsdp_size = lax.axis_size("fsdp")
    tp_size = lax.axis_size("tp")
    tp_index = lax.axis_index("tp")
    row_count, owned = tokens.shape
    full_width = gain.shape[0]
    rank = adapter_down_factors.shape[1]
    if tp_size == 2 and fsdp_size == 16 and grid_fits(weights, cots, tokens, rank):
        return grid_step(tokens, gain, weights, adapter_down_factors, ups, cots)

    def tp_sum(value):
        if tp_size != 2:
            return lax.psum(value, "tp")
        with jax.named_scope("pair_sum"):
            return value + lax.ppermute(value, "tp", [(0, 1), (1, 0)])

    wide = tokens.astype(jnp.float32)
    gain_own = lax.dynamic_slice_in_dim(gain, tp_index * owned, owned, 0)
    down = lax.dynamic_slice_in_dim(adapter_down_factors, tp_index * owned, owned, 2)
    down = down.reshape(3 * rank, owned)
    low_in = lax.dot_general(
        wide * gain_own[None, :],
        down.astype(jnp.float32),
        (((1,), (1,)), ((), ())),
        precision=lax.Precision.HIGHEST,
    )
    low_out = jnp.concatenate([transposed_product(c, u) for c, u in zip(cots, ups)], axis=1)
    squares = jnp.sum(wide * wide, axis=1, keepdims=True)
    small = tp_sum(jnp.concatenate([squares, low_in, low_out], axis=1))
    inverse = lax.rsqrt(small[:, :1] / full_width + norm_eps)
    in_low = (small[:, 1 : 1 + 3 * rank] * inverse).astype(jnp.bfloat16)
    out_low = small[:, 1 + 3 * rank :].astype(jnp.bfloat16)
    unit_rows = wide * inverse
    normed = (unit_rows * gain_own[None, :]).astype(jnp.bfloat16)
    scale = adapter_scale / math.sqrt(row_count * fsdp_size)

    def token_product(left, right):
        return scale * lax.dot_general(
            left, right, (((0,), (0,)), ((), ())), preferred_element_type=jnp.float32
        )

    down_local = token_product(out_low, normed)
    up_local = [
        token_product(in_low[:, rank * m : rank * (m + 1)], cots[m]) for m in range(3)
    ]
    small_work = tuple(down_local[rank * m : rank * (m + 1)] for m in range(3)) + tuple(up_local)
    back = plain_back(weights, cots, full_width)
    grads = lax.psum(jnp.concatenate(small_work, axis=1), "fsdp")
    grad_down = jnp.stack([grads[:, owned * m : owned * (m + 1)] for m in range(3)])
    ends = [3 * owned]
    for cot in cots:
        ends.append(ends[-1] + cot.shape[1])
    up_q, up_k, up_v = [grads[:, low:high] for low, high in zip(ends[:-1], ends[1:])]

    back = back + adapter_scale * jnp.dot(out_low, down, preferred_element_type=jnp.float32)
    gained = gain_own[None, :] * back
    inner = tp_sum(jnp.sum(gained * unit_rows, axis=1, keepdims=True)) / full_width
    grad_tokens = (inverse * (gained - unit_rows * inner)).astype(jnp.bfloat16)
    return (grad_tokens, grad_down, up_q, up_k, up_v)


def solution(mesh):
    in_specs = (
        P("fsdp", "tp"),
        P(),
        P("fsdp", "tp"),
        P("fsdp", "tp"),
        P("fsdp", "tp"),
        P(),
        P(None, "tp"),
        P(None, "tp"),
        P(None, "tp"),
        P("fsdp", "tp"),
        P("fsdp", "tp"),
        P("fsdp", "tp"),
    )
    out_specs = (P("fsdp", "tp"), P(None, None, "tp"), P(None, "tp"), P(None, "tp"), P(None, "tp"))
    step = jax.shard_map(shards, mesh=mesh, in_specs=in_specs, out_specs=out_specs, check_vma=False)
    return step
```

```python
import functools
import math

import jax
import jax.numpy as jnp
from jax import lax
from jax.experimental import pallas as pl
from jax.experimental.pallas import tpu as pltpu
from jax.sharding import PartitionSpec as P

norm_eps = 1e-05
adapter_scale = 2.0


def transposed_product(left, right):
    return lax.dot_general(
        left, right, (((1,), (1,)), ((), ())), preferred_element_type=jnp.float32
    )


def plain_back(weights, cotangents, full_width):
    total = jnp.zeros((cotangents[0].shape[0], full_width), jnp.float32)
    for weight, cotangent in zip(weights, cotangents):
        whole = lax.all_gather(weight, "fsdp", axis=0, tiled=True)
        total = total + transposed_product(cotangent, whole)
    return lax.psum_scatter(total, "tp", scatter_dimension=1, tiled=True)


def near_and_far_orders(count):
    near = list(range(count))
    every = list(range(2 * count))
    outer, outer_marks = [], {}
    inner, inner_marks = [], {}

    def add(order, marks, name, groups, ts):
        marks[name] = len(order)
        order.extend((w, t, n) for t in ts for w, n in groups)

    own, row = (0, 2), (2, 2)
    first, second = (4, 2), (6, 2)
    add(outer, outer_marks, "near", [own], near)
    add(outer, outer_marks, "f0", [(4, 1)], near)
    add(outer, outer_marks, "y", [row], near)
    add(outer, outer_marks, "f1", [(6, 1)], near)
    late = [(4, 1), (6, 1)]
    for i in range(count):
        add(outer, outer_marks, f"z{i}", [own, row] + late, [count + i])
        if i == count - 3:
            add(outer, outer_marks, "fy0", [(5, 1)], range(count + i + 1))
            late = [first, (6, 1)]
        if i == count - 2:
            add(outer, outer_marks, "fy1", [(7, 1)], range(count + i + 1))
            late = [first, second]
    add(inner, inner_marks, "near", [own], near)
    for i in range(count):
        add(inner, inner_marks, f"z{i}", [own], [count + i])
    add(inner, inner_marks, "y", [row], every)
    add(inner, inner_marks, "f0", [(4, 1)], every)
    add(inner, inner_marks, "fy0", [(5, 1)], every)
    add(inner, inner_marks, "f1", [(6, 1)], every)
    add(inner, inner_marks, "fy1", [(7, 1)], every)
    steps = max(len(outer), len(inner))
    lengths = len(outer), len(inner)
    for order in (outer, inner):
        order.extend([(0, 0, 0)] * (steps - len(order)))
    return (outer, outer_marks), (inner, inner_marks), lengths


def packed(digits):
    words = []
    for low in range(0, len(digits), 10):
        words.append(sum(d << (3 * k) for k, d in enumerate(digits[low : low + 10])))
    return words


def digit_at(step, is_inner, outer_digits, inner_digits):
    word = jnp.int32(0)
    for k, (o, i) in enumerate(zip(packed(outer_digits), packed(inner_digits))):
        value = jnp.where(is_inner == 1, jnp.int32(i), jnp.int32(o))
        word = jnp.where(step // 10 == k, value, word)
    return lax.shift_right_logical(word, 3 * (step % 10)) % 8


def piece_rows(half):
    size = 48 if half > 48 else half
    cuts = list(range(0, half, size)) + [half]
    return list(zip(cuts[:-1], cuts[1:]))


def grid_kernel(
    settings,
    cq, ck, cv, wq, wk, wv, tokens, gain, adapters, uq, uk, uv,
    out, inner_out, inverse_out, grad_down, grad_up_q, grad_up_k, grad_up_v,
    W, C, S, X, R,
    T, GW, GA, U, D, GD, A, AR, INV, LO, ZT, N, B, I, IR,
    G, GC, GY, H, HZ, F, GDV, GQ, GK, GV, grad_sem,
    load_w, load_c, load_s, store_sem,
    a_send, a_recv, i_send, i_recv,
    gc_send, gc_recv, gy_send, gy_recv, gz_send, gz_recv, ga_send, ga_recv, gb_send, gb_recv, gd_send, gd_recv,
    cc_send, cc_recv, cz_send, cz_recv, zc_send, zc_recv,
    y_send, y_recv, far_send, far_recv, fy_send, fy_recv,
    x_send, x_recv, r_send, r_recv,
):
    half = W.shape[1]
    block = 2 * half
    count = C.shape[0] // 2
    lanes = R.shape[2]
    top = 8
    place = lax.axis_index("fsdp")
    side = lax.axis_index("tp")

    def flipped(bit):
        return place + bit * (1 - 2 * ((place // bit) % 2))

    def at(bit):
        return {"fsdp": flipped(bit), "tp": side}

    def both(one, two):
        return {"fsdp": flipped(one) + flipped(two) - place, "tp": side}

    core, row, near_z, far_z = at(1), at(2), at(4), at(8)
    diagonal, third_z = both(4, 1), both(4, 8)
    twin = {"fsdp": place, "tp": 1 - side}
    z = place // 4
    is_inner = ((z + 1) // 2) % 2
    keep_late = (place // top + side) % 2

    pieces = piece_rows(half)
    columns = []
    low = 0
    for ref in (cq, ck, cv):
        columns.append((low, low + ref.shape[1]))
        low += ref.shape[1]

    def load_cot(i, m):
        low, high = columns[m]
        ref = (cq, ck, cv)[m]
        return pltpu.make_async_copy(
            ref.at[pl.ds(i * lanes, lanes), :],
            C.at[i, pl.ds(0, lanes), pl.ds(low, high - low)],
            load_c.at[i, m],
        )

    def load_weight(h, m):
        low, high = columns[m]
        ref = (wq, wk, wv)[m]
        return pltpu.make_async_copy(
            ref.at[pl.ds(h * half, half), :],
            W.at[h, :, pl.ds(low, high - low)],
            load_w.at[h, m],
        )

    def remote(src, dst, send, recv, device):
        return pltpu.make_async_remote_copy(
            src_ref=src, dst_ref=dst, send_sem=send, recv_sem=recv,
            device_id=device, device_id_type=pl.DeviceIdType.MESH,
        )

    lower, upper = pl.ds(0, lanes), pl.ds(lanes, lanes)
    full_width, owned, rank, scale = settings
    own_columns = pl.ds(pl.multiple_of(side * owned, lanes), owned)
    feature_blocks = owned // lanes
    share = F.shape[0] // 2
    core_index, row_index = place % 2, (place // 2) % 2
    part_start = core_index * share + row_index * (share // 2)
    piece = share // 8

    small_loads = [
        pltpu.make_async_copy(tokens, T, load_s.at[0]),
        pltpu.make_async_copy(gain, GW, load_s.at[1]),
    ]
    for m in range(3):
        small_loads.append(
            pltpu.make_async_copy(
                adapters.at[m, :, own_columns], D.at[pl.ds(rank * m, rank)], load_s.at[2 + m]
            )
        )
        low, high = columns[m]
        small_loads.append(
            pltpu.make_async_copy(
                (uq, uk, uv)[m],
                U.at[pl.ds(rank * m, rank), pl.ds(low, high - low)],
                load_s.at[5 + m],
            )
        )

    def pair_rows():
        return remote(A, AR, a_send, a_recv, twin)

    def inner_rows(i):
        return remote(I.at[i], IR.at[i], i_send, i_recv.at[i], twin)

    def grads_core():
        away = (1 - core_index) * share
        return remote(G.at[pl.ds(away, share)], GC, gc_send, gc_recv, core)

    def grads_row():
        away = core_index * share + (1 - row_index) * (share // 2)
        return remote(G.at[pl.ds(away, share // 2)], GY, gy_send, gy_recv, row)

    z_partners = ((near_z, 1), (far_z, 2), (third_z, 3))

    def z_flip(bits):
        low, high = z % 2, z // 2
        low = 1 - low if bits % 2 else low
        high = 1 - high if bits // 2 else high
        return 2 * high + low

    def grads_z(n):
        device, bits = z_partners[n]
        return remote(
            H.at[pl.ds(z_flip(bits) * piece, piece)], HZ.at[n], gz_send, gz_recv.at[n], device
        )

    mine_z = pl.ds(part_start + z * piece, piece)
    mine_y = pl.ds(part_start, share // 2)
    mine_c = pl.ds(core_index * share, share)

    def spread_z(n):
        return remote(F.at[mine_z], F.at[mine_z], ga_send, ga_recv.at[n], z_partners[n][0])

    def spread_y():
        return remote(F.at[mine_y], F.at[mine_y], gb_send, gb_recv, row)

    def spread_c():
        return remote(F.at[mine_c], F.at[mine_c], gd_send, gd_recv, core)

    def cot_core(i):
        return remote(C.at[i, lower], C.at[i, upper], cc_send, cc_recv.at[i], core)

    def cot_z(i):
        return remote(C.at[i, lower], C.at[count + i, lower], cz_send, cz_recv.at[i], near_z)

    cot_pieces = [(i, low) for i in range(count) for low in range(0, lanes, 32)]

    def start_cot_pieces(low, high):
        for i, first in cot_pieces[low:high]:
            rows = pl.ds(first, 32)
            remote(
                C.at[i, rows], C.at[count + i, rows], cz_send, cz_recv.at[i], near_z
            ).start()

    def cot_zc(i):
        return remote(
            C.at[count + i, lower], C.at[count + i, upper], zc_send, zc_recv.at[i], core
        )

    def weight_y(h):
        return remote(W.at[h], W.at[2 + h], y_send, y_recv.at[h], row)

    def far(h, k):
        low, high = pieces[k]
        rows = pl.ds(low, high - low)
        return remote(W.at[h, rows], W.at[4 + 2 * h, rows], far_send, far_recv.at[h, k], far_z)

    def far_y(h, k):
        low, high = pieces[k]
        rows = pl.ds(low, high - low)
        return remote(W.at[4 + 2 * h, rows], W.at[5 + 2 * h, rows], fy_send, fy_recv.at[h, k], row)

    for i in range(count):
        for m in range(3):
            load_cot(i, m).start()
    for h in range(2):
        for m in range(3):
            load_weight(h, m).start()
    for copy in small_loads:
        copy.start()

    barrier = pltpu.get_barrier_semaphore()
    partners = (core, row, near_z, diagonal, far_z, third_z, twin)
    for partner in partners:
        pl.semaphore_signal(
            barrier, inc=1, device_id=partner, device_id_type=pl.DeviceIdType.MESH
        )
    pl.semaphore_wait(barrier, len(partners))

    for i in range(count):
        for m in range(3):
            load_cot(i, m).wait()

        @pl.when(is_inner == 0)
        def _():
            cot_z(i).start()

    for h in range(2):
        for m in range(3):
            load_weight(h, m).wait()

        @pl.when(is_inner == 1)
        def _():
            for k in range(len(pieces)):
                far(h, k).start()

        if h == 0:
            weight_y(h).start()
    for i in range(count):
        cot_core(i).start()

    lane = lax.broadcasted_iota(jnp.int32, (lanes, lanes), 1)
    used = 3 * rank
    D[pl.ds(used, lanes - used), :] = jnp.zeros((lanes - used, owned), jnp.bfloat16)
    U[pl.ds(used, lanes - used), :] = jnp.zeros((lanes - used, U.shape[1]), jnp.bfloat16)
    for m in range(3):
        for other in range(3):
            if other != m:
                low, high = columns[other]
                U[pl.ds(rank * m, rank), pl.ds(low, high - low)] = jnp.zeros(
                    (rank, high - low), jnp.bfloat16
                )
    for p in range(3):
        GD[p] = jnp.zeros((lanes, owned), jnp.bfloat16)
    for copy in small_loads:
        copy.wait()
    for j in range(feature_blocks):
        GA[:, pl.ds(j * lanes, lanes)] = GW[pl.ds(side * feature_blocks + j, 1), :]
    rest = D[pl.ds(0, used), :].astype(jnp.float32) * GA[...]
    for p in range(3):
        part = rest.astype(jnp.bfloat16)
        GD[p, pl.ds(64, used), :] = part
        rest = rest - part.astype(jnp.float32)

    def nt_dot(left, right):
        return lax.dot_general(
            left, right, (((1,), (1,)), ((), ())), preferred_element_type=jnp.float32
        )

    for i in range(count):
        rows = pl.ds(i * lanes, lanes)
        own_rows = T[rows, :]
        value = nt_dot(C[i, lower, :], U[...])
        for p in range(3):
            value = value + nt_dot(own_rows, GD[p])
        wide = own_rows.astype(jnp.float32)
        squares = jnp.sum(wide * wide, axis=1, keepdims=True)
        A[i] = value + jnp.where(lane == 120, squares, 0.0)
    pair_rows().start()
    pair_rows().wait_recv()
    for i in range(count):
        rows = pl.ds(i * lanes, lanes)
        both_sum = A[i] + AR[i]
        squares = jnp.sum(jnp.where(lane == 120, both_sum, 0.0), axis=1, keepdims=True)
        inverse = lax.rsqrt(squares / full_width + norm_eps)
        INV[i] = jnp.broadcast_to(inverse, (lanes, lanes))
        low = jnp.where(lane < used, both_sum, 0.0)
        LO[i] = low.astype(jnp.bfloat16)
        scaled = jnp.where((lane >= 64) & (lane < 64 + used), both_sum * inverse, 0.0)
        ZT[:, rows] = (low + scaled).T.astype(jnp.bfloat16)
        N[rows, :] = (T[rows, :].astype(jnp.float32) * inverse * GA[...]).astype(jnp.bfloat16)

    def down_block(j, carry):
        cols = pl.ds(pl.multiple_of(j * lanes, lanes), lanes)
        value = scale * jnp.dot(
            ZT[pl.ds(0, 64), :], N[:, cols], preferred_element_type=jnp.float32
        )
        for m in range(3):
            G[m * feature_blocks + j] = value[rank * m : rank * (m + 1)]
        return carry

    lax.fori_loop(0, feature_blocks, down_block, 0)
    first = 3 * feature_blocks
    for m in range(3):
        low, high = columns[m]

        def up_block(j, carry, m=m, low=low):
            cols = pl.ds(pl.multiple_of(low + j * lanes, lanes), lanes)
            value = jnp.zeros((rank, lanes), jnp.float32)
            for i in range(count):
                value = value + jnp.dot(
                    ZT[pl.ds(64 + rank * m, rank), pl.ds(i * lanes, lanes)],
                    C[i, lower, cols],
                    preferred_element_type=jnp.float32,
                )
            G[first + low // lanes + j] = scale * value
            return carry

        lax.fori_loop(0, (high - low) // lanes, up_block, 0)
    filled = first + columns[2][1] // lanes
    for j in range(filled, G.shape[0]):
        G[j] = jnp.zeros((rank, lanes), jnp.float32)
    grads_core().start()
    grads_core().wait_recv()
    G[mine_c] = G[mine_c] + GC[...]
    grads_row().start()
    weight_y(1).start()

    (outer, outer_marks), (inner, inner_marks), lengths = near_and_far_orders(count)
    tiles = is_inner * lengths[1] + (1 - is_inner) * lengths[0]
    lag = 3

    def order_at(step):
        return [
            digit_at(step, is_inner, [a[k] for a in outer], [a[k] for a in inner])
            for k in range(3)
        ]

    def when(step, outer_name, inner_name, inner_shift=0):
        o = outer_marks[outer_name] if outer_name else -1
        i = inner_marks[inner_name] + inner_shift if inner_name else -1
        return pl.when(step == is_inner * i + (1 - is_inner) * o)

    def take_far(h, k):
        far(h, k).wait_recv()
        far_y(h, k).start()

    last_outer = f"z{count - 1}"
    last_step = is_inner * inner_marks["f1"] + (1 - is_inner) * outer_marks[last_outer]
    waiting = is_inner * count + (1 - is_inner) * (count - 1)

    def sum_rows(slot):
        base = place % top
        other = keep_late * (slot % 2) + (1 - keep_late) * (slot // 2)
        part = keep_late * (slot // 2) + (1 - keep_late) * (slot % 2)
        index = base + other * 2 * (1 - 2 * ((base // 2) % 2))
        return pl.ds(pl.multiple_of(index * block + part * half, 16), half)

    def return_far(mine, t2, rows):
        i = t2 - count
        remote(S.at[mine, t2, 0], R.at[i, rows], r_send, r_recv.at[i], near_z).start()
        remote(S.at[mine, t2, 1], R.at[i, rows], r_send, r_recv.at[i], diagonal).start()

    def return_held(n, carry):
        slot, i = n % 4, n // 4
        return_far(slot, count + i, sum_rows(slot))
        return carry

    def body(step, carry):
        @when(step, "near", "near")
        def _():
            for i in range(count):
                cot_core(i).wait_recv()

        @when(step, None, f"z{count - 1}")
        def _():
            remote(W.at[pl.ds(0, 2)], W.at[pl.ds(4, 2)], far_send, far_recv.at[0, 0], far_z).wait_send()
            start_cot_pieces(0, 4)

        @when(step, "f0", "z1")
        def _():
            grads_row().wait_recv()
            G[mine_y] = G[mine_y] + GY[...]
            H[...] = G[mine_y].astype(jnp.bfloat16)
            for n in range(3):
                grads_z(n).start()

        @when(step, "y", None)
        def _():
            for k in range(len(pieces)):
                far(0, k).start()

        @when(step, "z0", "f0")
        def _():
            value = G[mine_z]
            for n in range(3):
                grads_z(n).wait_recv()
                value = value + HZ[n].astype(jnp.float32)
            F[mine_z] = value.astype(jnp.bfloat16)
            for n in range(3):
                spread_z(n).start()

        @when(step, "z0", None)
        def _():
            for k in range(len(pieces)):
                far(1, k).start()

        @when(step, last_outer, "fy1")
        def _():
            for n in range(3):
                spread_z(n).wait_recv()
            spread_y().start()

        for i in range(count):
            @when(step, f"z{i}", f"z{i}")
            def _():
                cot_z(i).wait_recv()
                cot_zc(i).start()
                cot_zc(i).wait_recv()

        @when(step, "y", "y")
        def _():
            weight_y(0).wait_recv()
            weight_y(1).wait_recv()

        number = len(pieces)

        @when(step, "f0", None)
        def _():
            for k in range(number):
                take_far(0, k)

        @when(step, "f1", None)
        def _():
            for k in range(number):
                take_far(1, k)

        @pl.when((step == last_step) & (keep_late == 0))
        def _():
            lax.fori_loop(0, 4 * waiting, return_held, 0)

        waves = number // 2
        extra = -(-(len(cot_pieces) - 4) // number)
        takes = [("f0", (k - number + 2) * 3 if k < number - 2 else 0) for k in range(number)]
        takes += [("fy0", 0)] * waves + [("f1", 0)] * (number - waves)
        for k, (name, shift) in enumerate(takes):
            @when(step, None, name, shift)
            def _():
                take_far(k // number, k % number)
                if k < number:
                    start_cot_pieces(4 + extra * k, 4 + extra * (k + 1))

        for h in range(2):
            @when(step, f"fy{h}", f"fy{h}")
            def _():
                for k in range(number):
                    far_y(h, k).wait_recv()

        w, t, n = order_at(step)

        def product(size):
            value = lax.dot_general(
                W[pl.ds(w, size)].reshape(size * half, W.shape[2]),
                C[t],
                (((1,), (1,)), ((), ())),
                preferred_element_type=jnp.float32,
            ).astype(jnp.bfloat16)
            for q in range(size):
                for part in range(2):
                    S[w + q, t, part] = value[
                        half * q : half * (q + 1), lanes * part : lanes * (part + 1)
                    ]

        @pl.when((step < tiles) & (n == 1))
        def _():
            product(1)

        @pl.when((step < tiles) & (n == 2))
        def _():
            product(2)

        for q in range(2):
            @pl.when((step < tiles) & (q < n) & (w // 4 != keep_late))
            def _():
                remote(
                    S.at[w + q, t], X.at[w % 4 + q, t], x_send, x_recv.at[w % 4 + q, t], twin
                ).start()

        back = jnp.maximum(step - lag, 0)
        w2, t2, n2 = order_at(back)

        for q in range(2):
            @pl.when((step >= lag) & (step < tiles + lag) & (q < n2) & (w2 // 4 == keep_late))
            def _():
                mine, slot = w2 + q, w2 % 4 + q
                remote(
                    S.at[mine, t2], X.at[slot, t2], x_send, x_recv.at[slot, t2], twin
                ).wait_recv()
                total = S[mine, t2].astype(jnp.float32) + X[slot, t2].astype(jnp.float32)
                S[mine, t2] = total.astype(jnp.bfloat16)
                rows = sum_rows(slot)
                i = t2 % count

                @pl.when(t2 < count)
                def _():
                    R[i, rows, :] = total[0].astype(jnp.bfloat16)
                    remote(S.at[mine, t2, 1], R.at[i, rows], r_send, r_recv.at[i], core).start()

                @pl.when((t2 >= count) & ((keep_late == 1) | (t2 >= count + waiting)))
                def _():
                    return_far(mine, t2, rows)

        return carry

    lax.fori_loop(0, max(lengths) + lag, body, 0)

    spread_y().wait_recv()
    spread_c().start()
    spread_c().wait_recv()
    for j in range(feature_blocks):
        for m in range(3):
            GDV[m, :, pl.ds(j * lanes, lanes)] = F[m * feature_blocks + j].astype(jnp.float32)
    for m, ref in enumerate((GQ, GK, GV)):
        low, high = columns[m]
        for j in range((high - low) // lanes):
            ref[:, pl.ds(j * lanes, lanes)] = F[first + low // lanes + j].astype(jnp.float32)
    part = pl.ds(0, 3 * R.shape[1] // 4)
    stores = [
        pltpu.make_async_copy(source, target, grad_sem.at[k])
        for k, (source, target) in enumerate(
            zip((GDV, GQ, GK, GV), (grad_down, grad_up_q, grad_up_k, grad_up_v))
        )
    ]
    for i in range(count):
        inverse_out[pl.ds(i * lanes, lanes), :] = INV[i]
    for store in stores:
        store.start()
    for i in range(count):
        rows = pl.ds(i * lanes, lanes)
        remote(R.at[i, part], R.at[i, part], r_send, r_recv.at[i], core).wait_recv()
        inverse = INV[i]

        def gained_block(j, carry, i=i, rows=rows, inverse=inverse):
            cols = pl.ds(pl.multiple_of(j * lanes, lanes), lanes)
            back = R[i, cols, :].astype(jnp.float32).T
            back = back + adapter_scale * jnp.dot(
                LO[i], D[:, cols], preferred_element_type=jnp.float32
            )
            gained = GA[:, cols] * back
            B[rows, cols] = gained
            return carry + gained * (T[rows, cols].astype(jnp.float32) * inverse)

        total = lax.fori_loop(
            0, feature_blocks, gained_block, jnp.zeros((lanes, lanes), jnp.float32), unroll=11
        )
        I[i] = jnp.broadcast_to(jnp.sum(total, axis=1, keepdims=True), (lanes, lanes))
        inner_rows(i).start()
        stores.append(pltpu.make_async_copy(B.at[rows], out.at[rows], store_sem.at[i]))
        stores[-1].start()
    for i in range(count):
        rows = pl.ds(i * lanes, lanes)
        inner_rows(i).wait_recv()
        inner_out[rows, :] = (I[i] + IR[i]) / full_width

    results = remote(R.at[:, part], R.at[:, part], r_send, r_recv.at[0], core)
    results.wait_send()
    own = C.at[pl.ds(0, count), lower]
    remote(own, own, cc_send, cc_recv.at[0], core).wait_send()
    remote(own, own, cz_send, cz_recv.at[0], core).wait_send()
    remote(own, own, zc_send, zc_recv.at[0], core).wait_send()
    two = W.at[pl.ds(0, 2)]
    remote(two, two, y_send, y_recv.at[0], core).wait_send()

    @pl.when(is_inner == 0)
    def _():
        remote(two, two, far_send, far_recv.at[0, 0], core).wait_send()

    remote(two, two, fy_send, fy_recv.at[0, 0], core).wait_send()
    four = S.at[pl.ds(0, 4)]
    remote(four, four, x_send, x_recv.at[0, 0], core).wait_send()
    pair_rows().wait_send()
    remote(I, I, i_send, i_recv.at[0], twin).wait_send()
    grads_core().wait_send()
    grads_row().wait_send()
    three = H.at[pl.ds(0, 3 * piece)]
    remote(three, three, gz_send, gz_recv.at[0], core).wait_send()
    three = F.at[pl.ds(0, 3 * piece)]
    remote(three, three, ga_send, ga_recv.at[0], core).wait_send()
    spread_y().wait_send()
    spread_c().wait_send()
    for store in stores:
        store.wait()


token_lanes = 128


def final_kernel(gained, tokens, inner, inverse, *refs):
    grads, (out, *grad_outs) = refs[:4], refs[4:]

    @pl.when(pl.program_id(0) == 0)
    def _():
        for source, target in zip(grads, grad_outs):
            target[...] = source[...]

    scale = inverse[:, :1]
    unit = tokens[...].astype(jnp.float32) * scale
    out[...] = (scale * (gained[...] - unit * inner[:, :1])).astype(out.dtype)


def grid_fits(weights, cotangents, tokens, rank):
    rows = weights[0].shape[0]
    tokens_here, owned = tokens.shape
    count = tokens_here // token_lanes
    aligned = all(c.shape[1] % token_lanes == 0 for c in cotangents) and owned % token_lanes == 0
    return (
        aligned and rows % 32 == 0 and tokens_here % token_lanes == 0
        and count in (3, 4) and rank == 16 and owned == 8 * rows
    )


def grid_step(tokens, gain, weights, adapters, ups, cotangents):
    rows = weights[0].shape[0]
    tokens_here, owned = tokens.shape
    full_width = gain.shape[0]
    rank = adapters.shape[1]
    depth = sum(w.shape[1] for w in weights)
    half = rows // 2
    lanes = token_lanes
    count = tokens_here // lanes
    number = len(piece_rows(half))
    scale = adapter_scale / math.sqrt(tokens_here * lax.axis_size("fsdp"))
    grad_blocks = 16 * -(-(3 * owned + depth) // (16 * lanes))
    share = grad_blocks // 2
    DMA = pltpu.SemaphoreType.DMA
    f32, bf16 = jnp.float32, jnp.bfloat16
    vmem = pl.BlockSpec(memory_space=pltpu.VMEM)
    gained, inner, inverse, *grads = pl.pallas_call(
        functools.partial(grid_kernel, (full_width, owned, rank, scale)),
        out_shape=(
            jax.ShapeDtypeStruct(tokens.shape, f32),
            jax.ShapeDtypeStruct((tokens_here, lanes), f32),
            jax.ShapeDtypeStruct((tokens_here, lanes), f32),
            jax.ShapeDtypeStruct((3, rank, owned), f32),
        ) + tuple(jax.ShapeDtypeStruct((rank, c.shape[1]), f32) for c in cotangents),
        in_specs=[pl.BlockSpec(memory_space=pl.ANY)] * 12,
        out_specs=(pl.BlockSpec(memory_space=pl.ANY),) + (vmem,) * 2
        + (pl.BlockSpec(memory_space=pl.ANY),) * 4,
        scratch_shapes=[
            pltpu.VMEM((8, half, depth), bf16),
            pltpu.VMEM((2 * count, 2 * lanes, depth), bf16),
            pltpu.VMEM((8, 2 * count, 2, half, lanes), bf16),
            pltpu.VMEM((4, 2 * count, 2, half, lanes), bf16),
            pltpu.VMEM((count, 8 * rows, lanes), bf16),
            pltpu.VMEM((tokens_here, owned), bf16),
            pltpu.VMEM((full_width // lanes, lanes), f32),
            pltpu.VMEM((1, owned), f32),
            pltpu.VMEM((lanes, depth), bf16),
            pltpu.VMEM((lanes, owned), bf16),
            pltpu.VMEM((3, lanes, owned), bf16),
            pltpu.VMEM((count, lanes, lanes), f32),
            pltpu.VMEM((count, lanes, lanes), f32),
            pltpu.VMEM((count, lanes, lanes), f32),
            pltpu.VMEM((count, lanes, lanes), bf16),
            pltpu.VMEM((lanes, tokens_here), bf16),
            pltpu.VMEM((tokens_here, owned), bf16),
            pltpu.VMEM((tokens_here, owned), f32),
            pltpu.VMEM((count, lanes, lanes), f32),
            pltpu.VMEM((count, lanes, lanes), f32),
            pltpu.VMEM((grad_blocks, rank, lanes), f32),
            pltpu.VMEM((share, rank, lanes), f32),
            pltpu.VMEM((share // 2, rank, lanes), f32),
            pltpu.VMEM((share // 2, rank, lanes), bf16),
            pltpu.VMEM((3, share // 8, rank, lanes), bf16),
            pltpu.VMEM((grad_blocks, rank, lanes), bf16),
            pltpu.VMEM((3, rank, owned), f32),
            *[pltpu.VMEM((rank, c.shape[1]), f32) for c in cotangents],
            DMA((4,)),
            DMA((2, 3)), DMA((count, 3)), DMA((8,)), DMA((count,)),
            DMA, DMA, DMA, DMA((count,)),
            DMA, DMA, DMA, DMA, DMA, DMA((3,)), DMA, DMA((3,)), DMA, DMA, DMA, DMA,
            DMA, DMA((count,)), DMA, DMA((count,)), DMA, DMA((count,)),
            DMA, DMA((2,)), DMA, DMA((2, number)), DMA, DMA((2, number)),
            DMA, DMA((4, 2 * count)), DMA, DMA((count,)),
        ],
        compiler_params=pltpu.CompilerParams(
            collective_id=0, has_side_effects=True, vmem_limit_bytes=60 * 1024 * 1024
        ),
        cost_estimate=pl.CostEstimate(
            flops=2 * 16 * rows * tokens_here * depth, bytes_accessed=2 * 8 * rows * depth,
            transcendentals=0,
        ),
        name="grid",
    )(*cotangents, *weights, tokens, gain.reshape(full_width // lanes, lanes), adapters, *ups)
    step_rows = tokens_here // 2

    def by_rows(width):
        return pl.BlockSpec((step_rows, width), lambda i: (i, 0))

    whole = [pl.BlockSpec(g.shape, lambda i, k=len(g.shape): (0,) * k) for g in grads]
    return pl.pallas_call(
        final_kernel,
        grid=(tokens_here // step_rows,),
        out_shape=(jax.ShapeDtypeStruct(tokens.shape, bf16),)
        + tuple(jax.ShapeDtypeStruct(g.shape, f32) for g in grads),
        in_specs=[by_rows(owned), by_rows(owned), by_rows(lanes), by_rows(lanes), *whole],
        out_specs=(by_rows(owned), *whole),
        cost_estimate=pl.CostEstimate(
            flops=4 * tokens_here * owned, bytes_accessed=8 * tokens_here * owned, transcendentals=0
        ),
        name="final",
    )(gained, tokens, inner, inverse, *grads)


def shards(
    tokens,
    gain,
    query_projection_weight,
    key_projection_weight,
    value_projection_weight,
    adapter_down_factors,
    query_adapter_up,
    key_adapter_up,
    value_adapter_up,
    query_cotangent,
    key_cotangent,
    value_cotangent,
):
    return device_work(
        tokens,
        gain,
        (query_projection_weight, key_projection_weight, value_projection_weight),
        adapter_down_factors,
        (query_adapter_up, key_adapter_up, value_adapter_up),
        (query_cotangent, key_cotangent, value_cotangent),
    )


def device_work(tokens, gain, weights, adapter_down_factors, ups, cots):
    fsdp_size = lax.axis_size("fsdp")
    tp_size = lax.axis_size("tp")
    tp_index = lax.axis_index("tp")
    row_count, owned = tokens.shape
    full_width = gain.shape[0]
    rank = adapter_down_factors.shape[1]
    if tp_size == 2 and fsdp_size == 16 and grid_fits(weights, cots, tokens, rank):
        return grid_step(tokens, gain, weights, adapter_down_factors, ups, cots)

    def tp_sum(value):
        if tp_size != 2:
            return lax.psum(value, "tp")
        with jax.named_scope("pair_sum"):
            return value + lax.ppermute(value, "tp", [(0, 1), (1, 0)])

    wide = tokens.astype(jnp.float32)
    gain_own = lax.dynamic_slice_in_dim(gain, tp_index * owned, owned, 0)
    down = lax.dynamic_slice_in_dim(adapter_down_factors, tp_index * owned, owned, 2)
    down = down.reshape(3 * rank, owned)
    low_in = lax.dot_general(
        wide * gain_own[None, :],
        down.astype(jnp.float32),
        (((1,), (1,)), ((), ())),
        precision=lax.Precision.HIGHEST,
    )
    low_out = jnp.concatenate([transposed_product(c, u) for c, u in zip(cots, ups)], axis=1)
    squares = jnp.sum(wide * wide, axis=1, keepdims=True)
    small = tp_sum(jnp.concatenate([squares, low_in, low_out], axis=1))
    inverse = lax.rsqrt(small[:, :1] / full_width + norm_eps)
    in_low = (small[:, 1 : 1 + 3 * rank] * inverse).astype(jnp.bfloat16)
    out_low = small[:, 1 + 3 * rank :].astype(jnp.bfloat16)
    unit_rows = wide * inverse
    normed = (unit_rows * gain_own[None, :]).astype(jnp.bfloat16)
    scale = adapter_scale / math.sqrt(row_count * fsdp_size)

    def token_product(left, right):
        return scale * lax.dot_general(
            left, right, (((0,), (0,)), ((), ())), preferred_element_type=jnp.float32
        )

    down_local = token_product(out_low, normed)
    up_local = [
        token_product(in_low[:, rank * m : rank * (m + 1)], cots[m]) for m in range(3)
    ]
    small_work = tuple(down_local[rank * m : rank * (m + 1)] for m in range(3)) + tuple(up_local)
    back = plain_back(weights, cots, full_width)
    grads = lax.psum(jnp.concatenate(small_work, axis=1), "fsdp")
    grad_down = jnp.stack([grads[:, owned * m : owned * (m + 1)] for m in range(3)])
    ends = [3 * owned]
    for cot in cots:
        ends.append(ends[-1] + cot.shape[1])
    up_q, up_k, up_v = [grads[:, low:high] for low, high in zip(ends[:-1], ends[1:])]

    back = back + adapter_scale * jnp.dot(out_low, down, preferred_element_type=jnp.float32)
    gained = gain_own[None, :] * back
    inner = tp_sum(jnp.sum(gained * unit_rows, axis=1, keepdims=True)) / full_width
    grad_tokens = (inverse * (gained - unit_rows * inner)).astype(jnp.bfloat16)
    return (grad_tokens, grad_down, up_q, up_k, up_v)


def solution(mesh):
    in_specs = (
        P("fsdp", "tp"),
        P(),
        P("fsdp", "tp"),
        P("fsdp", "tp"),
        P("fsdp", "tp"),
        P(),
        P(None, "tp"),
        P(None, "tp"),
        P(None, "tp"),
        P("fsdp", "tp"),
        P("fsdp", "tp"),
        P("fsdp", "tp"),
    )
    out_specs = (P("fsdp", "tp"), P(None, None, "tp"), P(None, "tp"), P(None, "tp"), P(None, "tp"))
    step = jax.shard_map(shards, mesh=mesh, in_specs=in_specs, out_specs=out_specs, check_vma=False)
    return step
```

```python
import functools
import math

import jax
import jax.numpy as jnp
from jax import lax
from jax.experimental import pallas as pl
from jax.experimental.pallas import tpu as pltpu
from jax.sharding import PartitionSpec as P

norm_eps = 1e-05
adapter_scale = 2.0


def transposed_product(left, right):
    return lax.dot_general(
        left, right, (((1,), (1,)), ((), ())), preferred_element_type=jnp.float32
    )


def plain_back(weights, cotangents, full_width):
    total = jnp.zeros((cotangents[0].shape[0], full_width), jnp.float32)
    for weight, cotangent in zip(weights, cotangents):
        whole = lax.all_gather(weight, "fsdp", axis=0, tiled=True)
        total = total + transposed_product(cotangent, whole)
    return lax.psum_scatter(total, "tp", scatter_dimension=1, tiled=True)


def near_and_far_orders(count):
    near = list(range(count))
    every = list(range(2 * count))
    outer, outer_marks = [], {}
    inner, inner_marks = [], {}

    def add(order, marks, name, groups, ts):
        marks[name] = len(order)
        order.extend((w, t, n) for t in ts for w, n in groups)

    own, row = (0, 2), (2, 2)
    first, second = (4, 2), (6, 2)
    add(outer, outer_marks, "near", [own], near)
    add(outer, outer_marks, "f0", [(4, 1)], near)
    add(outer, outer_marks, "y", [row], near)
    add(outer, outer_marks, "f1", [(6, 1)], near)
    late = [(4, 1), (6, 1)]
    for i in range(count):
        add(outer, outer_marks, f"z{i}", [own, row] + late, [count + i])
        if i == count - 3:
            add(outer, outer_marks, "fy0", [(5, 1)], range(count + i + 1))
            late = [first, (6, 1)]
        if i == count - 2:
            add(outer, outer_marks, "fy1", [(7, 1)], range(count + i + 1))
            late = [first, second]
    add(inner, inner_marks, "near", [own], near)
    for i in range(count):
        add(inner, inner_marks, f"z{i}", [own], [count + i])
    add(inner, inner_marks, "y", [row], every)
    add(inner, inner_marks, "f0", [(4, 1)], every)
    add(inner, inner_marks, "fy0", [(5, 1)], every)
    add(inner, inner_marks, "f1", [(6, 1)], every)
    add(inner, inner_marks, "fy1", [(7, 1)], every)
    steps = max(len(outer), len(inner))
    lengths = len(outer), len(inner)
    for order in (outer, inner):
        order.extend([(0, 0, 0)] * (steps - len(order)))
    return (outer, outer_marks), (inner, inner_marks), lengths


def packed(digits):
    words = []
    for low in range(0, len(digits), 10):
        words.append(sum(d << (3 * k) for k, d in enumerate(digits[low : low + 10])))
    return words


def digit_at(step, is_inner, outer_digits, inner_digits):
    word = jnp.int32(0)
    for k, (o, i) in enumerate(zip(packed(outer_digits), packed(inner_digits))):
        value = jnp.where(is_inner == 1, jnp.int32(i), jnp.int32(o))
        word = jnp.where(step // 10 == k, value, word)
    return lax.shift_right_logical(word, 3 * (step % 10)) % 8


def piece_rows(half):
    size = 48 if half > 48 else half
    cuts = list(range(0, half, size)) + [half]
    return list(zip(cuts[:-1], cuts[1:]))


def grid_kernel(
    settings,
    cq, ck, cv, wq, wk, wv, tokens, gain, adapters, uq, uk, uv,
    out, inner_out, inverse_out, grad_down, grad_up_q, grad_up_k, grad_up_v,
    W, C, S, X, R,
    T, GW, GA, U, D, GD, A, AR, INV, LO, ZT, N, B, I, IR,
    G, GC, GY, H, HZ, F, GDV, GQ, GK, GV, grad_sem,
    load_w, load_c, load_s, store_sem,
    a_send, a_recv, i_send, i_recv,
    gc_send, gc_recv, gy_send, gy_recv, gz_send, gz_recv, ga_send, ga_recv, gb_send, gb_recv, gd_send, gd_recv,
    cc_send, cc_recv, cz_send, cz_recv, zc_send, zc_recv,
    y_send, y_recv, far_send, far_recv, fy_send, fy_recv,
    x_send, x_recv, r_send, r_recv,
):
    half = W.shape[1]
    block = 2 * half
    count = C.shape[0] // 2
    lanes = R.shape[2]
    top = 8
    place = lax.axis_index("fsdp")
    side = lax.axis_index("tp")

    def flipped(bit):
        return place + bit * (1 - 2 * ((place // bit) % 2))

    def at(bit):
        return {"fsdp": flipped(bit), "tp": side}

    def both(one, two):
        return {"fsdp": flipped(one) + flipped(two) - place, "tp": side}

    core, row, near_z, far_z = at(1), at(2), at(4), at(8)
    diagonal, third_z = both(4, 1), both(4, 8)
    twin = {"fsdp": place, "tp": 1 - side}
    z = place // 4
    is_inner = ((z + 1) // 2) % 2
    keep_late = (place // top + side) % 2

    pieces = piece_rows(half)
    columns = []
    low = 0
    for ref in (cq, ck, cv):
        columns.append((low, low + ref.shape[1]))
        low += ref.shape[1]

    def load_cot(i, m):
        low, high = columns[m]
        ref = (cq, ck, cv)[m]
        return pltpu.make_async_copy(
            ref.at[pl.ds(i * lanes, lanes), :],
            C.at[i, pl.ds(0, lanes), pl.ds(low, high - low)],
            load_c.at[i, m],
        )

    def load_weight(h, m):
        low, high = columns[m]
        ref = (wq, wk, wv)[m]
        return pltpu.make_async_copy(
            ref.at[pl.ds(h * half, half), :],
            W.at[h, :, pl.ds(low, high - low)],
            load_w.at[h, m],
        )

    def remote(src, dst, send, recv, device):
        return pltpu.make_async_remote_copy(
            src_ref=src, dst_ref=dst, send_sem=send, recv_sem=recv,
            device_id=device, device_id_type=pl.DeviceIdType.MESH,
        )

    lower, upper = pl.ds(0, lanes), pl.ds(lanes, lanes)
    full_width, owned, rank, scale = settings
    own_columns = pl.ds(pl.multiple_of(side * owned, lanes), owned)
    feature_blocks = owned // lanes
    share = F.shape[0] // 2
    core_index, row_index = place % 2, (place // 2) % 2
    part_start = core_index * share + row_index * (share // 2)
    piece = share // 8

    small_loads = [
        pltpu.make_async_copy(tokens, T, load_s.at[0]),
        pltpu.make_async_copy(gain, GW, load_s.at[1]),
    ]
    for m in range(3):
        small_loads.append(
            pltpu.make_async_copy(
                adapters.at[m, :, own_columns], D.at[pl.ds(rank * m, rank)], load_s.at[2 + m]
            )
        )
        low, high = columns[m]
        small_loads.append(
            pltpu.make_async_copy(
                (uq, uk, uv)[m],
                U.at[pl.ds(rank * m, rank), pl.ds(low, high - low)],
                load_s.at[5 + m],
            )
        )

    def pair_rows():
        return remote(A, AR, a_send, a_recv, twin)

    def inner_rows(i):
        return remote(I.at[i], IR.at[i], i_send, i_recv.at[i], twin)

    def grads_core():
        away = (1 - core_index) * share
        return remote(G.at[pl.ds(away, share)], GC, gc_send, gc_recv, core)

    def grads_row():
        away = core_index * share + (1 - row_index) * (share // 2)
        return remote(G.at[pl.ds(away, share // 2)], GY, gy_send, gy_recv, row)

    z_partners = ((near_z, 1), (far_z, 2), (third_z, 3))

    def z_flip(bits):
        low, high = z % 2, z // 2
        low = 1 - low if bits % 2 else low
        high = 1 - high if bits // 2 else high
        return 2 * high + low

    def grads_z(n):
        device, bits = z_partners[n]
        return remote(
            H.at[pl.ds(z_flip(bits) * piece, piece)], HZ.at[n], gz_send, gz_recv.at[n], device
        )

    mine_z = pl.ds(part_start + z * piece, piece)
    mine_y = pl.ds(part_start, share // 2)
    mine_c = pl.ds(core_index * share, share)

    def spread_z(n):
        return remote(F.at[mine_z], F.at[mine_z], ga_send, ga_recv.at[n], z_partners[n][0])

    def spread_y():
        return remote(F.at[mine_y], F.at[mine_y], gb_send, gb_recv, row)

    def spread_c():
        return remote(F.at[mine_c], F.at[mine_c], gd_send, gd_recv, core)

    def cot_core(i):
        return remote(C.at[i, lower], C.at[i, upper], cc_send, cc_recv.at[i], core)

    def cot_z(i):
        return remote(C.at[i, lower], C.at[count + i, lower], cz_send, cz_recv.at[i], near_z)

    cot_pieces = [(i, low) for i in range(count) for low in range(0, lanes, 32)]

    def start_cot_pieces(low, high):
        for i, first in cot_pieces[low:high]:
            rows = pl.ds(first, 32)
            remote(
                C.at[i, rows], C.at[count + i, rows], cz_send, cz_recv.at[i], near_z
            ).start()

    def cot_zc(i):
        return remote(
            C.at[count + i, lower], C.at[count + i, upper], zc_send, zc_recv.at[i], core
        )

    def weight_y(h):
        return remote(W.at[h], W.at[2 + h], y_send, y_recv.at[h], row)

    def far(h, k):
        low, high = pieces[k]
        rows = pl.ds(low, high - low)
        return remote(W.at[h, rows], W.at[4 + 2 * h, rows], far_send, far_recv.at[h, k], far_z)

    def far_y(h, k):
        low, high = pieces[k]
        rows = pl.ds(low, high - low)
        return remote(W.at[4 + 2 * h, rows], W.at[5 + 2 * h, rows], fy_send, fy_recv.at[h, k], row)

    for i in range(count):
        for m in range(3):
            load_cot(i, m).start()
    for h in range(2):
        for m in range(3):
            load_weight(h, m).start()
    for copy in small_loads:
        copy.start()

    barrier = pltpu.get_barrier_semaphore()
    partners = (core, row, near_z, diagonal, far_z, third_z, twin)
    for partner in partners:
        pl.semaphore_signal(
            barrier, inc=1, device_id=partner, device_id_type=pl.DeviceIdType.MESH
        )
    pl.semaphore_wait(barrier, len(partners))

    for i in range(count):
        for m in range(3):
            load_cot(i, m).wait()

        @pl.when(is_inner == 0)
        def _():
            cot_z(i).start()

    for h in range(2):
        for m in range(3):
            load_weight(h, m).wait()

        @pl.when(is_inner == 1)
        def _():
            for k in range(len(pieces)):
                far(h, k).start()

        if h == 0:
            weight_y(h).start()
    for i in range(count):
        cot_core(i).start()

    lane = lax.broadcasted_iota(jnp.int32, (lanes, lanes), 1)
    used = 3 * rank
    D[pl.ds(used, lanes - used), :] = jnp.zeros((lanes - used, owned), jnp.bfloat16)
    U[pl.ds(used, lanes - used), :] = jnp.zeros((lanes - used, U.shape[1]), jnp.bfloat16)
    for m in range(3):
        for other in range(3):
            if other != m:
                low, high = columns[other]
                U[pl.ds(rank * m, rank), pl.ds(low, high - low)] = jnp.zeros(
                    (rank, high - low), jnp.bfloat16
                )
    for p in range(3):
        GD[p] = jnp.zeros((lanes, owned), jnp.bfloat16)
    for copy in small_loads:
        copy.wait()
    for j in range(feature_blocks):
        GA[:, pl.ds(j * lanes, lanes)] = GW[pl.ds(side * feature_blocks + j, 1), :]
    rest = D[pl.ds(0, used), :].astype(jnp.float32) * GA[...]
    for p in range(3):
        part = rest.astype(jnp.bfloat16)
        GD[p, pl.ds(64, used), :] = part
        rest = rest - part.astype(jnp.float32)

    def nt_dot(left, right):
        return lax.dot_general(
            left, right, (((1,), (1,)), ((), ())), preferred_element_type=jnp.float32
        )

    for i in range(count):
        rows = pl.ds(i * lanes, lanes)
        own_rows = T[rows, :]
        value = nt_dot(C[i, lower, :], U[...])
        for p in range(3):
            value = value + nt_dot(own_rows, GD[p])
        wide = own_rows.astype(jnp.float32)
        squares = jnp.sum(wide * wide, axis=1, keepdims=True)
        A[i] = value + jnp.where(lane == 120, squares, 0.0)
    pair_rows().start()
    pair_rows().wait_recv()
    for i in range(count):
        rows = pl.ds(i * lanes, lanes)
        both_sum = A[i] + AR[i]
        squares = jnp.sum(jnp.where(lane == 120, both_sum, 0.0), axis=1, keepdims=True)
        inverse = lax.rsqrt(squares / full_width + norm_eps)
        INV[i] = jnp.broadcast_to(inverse, (lanes, lanes))
        low = jnp.where(lane < used, both_sum, 0.0)
        LO[i] = low.astype(jnp.bfloat16)
        scaled = jnp.where((lane >= 64) & (lane < 64 + used), both_sum * inverse, 0.0)
        ZT[:, rows] = (low + scaled).T.astype(jnp.bfloat16)
        N[rows, :] = (T[rows, :].astype(jnp.float32) * inverse * GA[...]).astype(jnp.bfloat16)

    def down_block(j, carry):
        cols = pl.ds(pl.multiple_of(j * lanes, lanes), lanes)
        value = scale * jnp.dot(
            ZT[pl.ds(0, 64), :], N[:, cols], preferred_element_type=jnp.float32
        )
        for m in range(3):
            G[m * feature_blocks + j] = value[rank * m : rank * (m + 1)]
        return carry

    lax.fori_loop(0, feature_blocks, down_block, 0)
    first = 3 * feature_blocks
    for m in range(3):
        low, high = columns[m]

        def up_block(j, carry, m=m, low=low):
            cols = pl.ds(pl.multiple_of(low + j * lanes, lanes), lanes)
            value = jnp.zeros((rank, lanes), jnp.float32)
            for i in range(count):
                value = value + jnp.dot(
                    ZT[pl.ds(64 + rank * m, rank), pl.ds(i * lanes, lanes)],
                    C[i, lower, cols],
                    preferred_element_type=jnp.float32,
                )
            G[first + low // lanes + j] = scale * value
            return carry

        lax.fori_loop(0, (high - low) // lanes, up_block, 0)
    filled = first + columns[2][1] // lanes
    for j in range(filled, G.shape[0]):
        G[j] = jnp.zeros((rank, lanes), jnp.float32)
    grads_core().start()
    grads_core().wait_recv()
    G[mine_c] = G[mine_c] + GC[...]
    grads_row().start()
    weight_y(1).start()

    (outer, outer_marks), (inner, inner_marks), lengths = near_and_far_orders(count)
    tiles = is_inner * lengths[1] + (1 - is_inner) * lengths[0]
    lag = 3

    def order_at(step):
        return [
            digit_at(step, is_inner, [a[k] for a in outer], [a[k] for a in inner])
            for k in range(3)
        ]

    def when(step, outer_name, inner_name, inner_shift=0):
        o = outer_marks[outer_name] if outer_name else -1
        i = inner_marks[inner_name] + inner_shift if inner_name else -1
        return pl.when(step == is_inner * i + (1 - is_inner) * o)

    def take_far(h, k):
        far(h, k).wait_recv()
        far_y(h, k).start()

    last_outer = f"z{count - 1}"
    last_step = is_inner * inner_marks["f1"] + (1 - is_inner) * (outer_marks["fy1"] + 1)
    waiting = is_inner * count + (1 - is_inner) * (count - 1)

    def sum_rows(slot):
        base = place % top
        other = keep_late * (slot % 2) + (1 - keep_late) * (slot // 2)
        part = keep_late * (slot // 2) + (1 - keep_late) * (slot % 2)
        index = base + other * 2 * (1 - 2 * ((base // 2) % 2))
        return pl.ds(pl.multiple_of(index * block + part * half, 16), half)

    def return_far(mine, t2, rows):
        i = t2 - count
        remote(S.at[mine, t2, 0], R.at[i, rows], r_send, r_recv.at[i], near_z).start()
        remote(S.at[mine, t2, 1], R.at[i, rows], r_send, r_recv.at[i], diagonal).start()

    def return_held(n, carry):
        slot, i = n % 4, n // 4
        return_far(slot, count + i, sum_rows(slot))
        return carry

    def body(step, carry):
        @when(step, "near", "near")
        def _():
            for i in range(count):
                cot_core(i).wait_recv()

        @when(step, None, f"z{count - 1}")
        def _():
            remote(W.at[pl.ds(0, 2)], W.at[pl.ds(4, 2)], far_send, far_recv.at[0, 0], far_z).wait_send()
            start_cot_pieces(0, 4)

        @when(step, "f0", "z1")
        def _():
            grads_row().wait_recv()
            G[mine_y] = G[mine_y] + GY[...]
            H[...] = G[mine_y].astype(jnp.bfloat16)
            for n in range(3):
                grads_z(n).start()

        @when(step, "y", None)
        def _():
            for k in range(len(pieces)):
                far(0, k).start()

        @when(step, "z0", "f0")
        def _():
            value = G[mine_z]
            for n in range(3):
                grads_z(n).wait_recv()
                value = value + HZ[n].astype(jnp.float32)
            F[mine_z] = value.astype(jnp.bfloat16)
            for n in range(3):
                spread_z(n).start()

        @when(step, "z0", None)
        def _():
            for k in range(len(pieces)):
                far(1, k).start()

        @when(step, last_outer, "fy1")
        def _():
            for n in range(3):
                spread_z(n).wait_recv()
            spread_y().start()

        for i in range(count):
            @when(step, f"z{i}", f"z{i}")
            def _():
                cot_z(i).wait_recv()
                cot_zc(i).start()
                cot_zc(i).wait_recv()

        @when(step, "y", "y")
        def _():
            weight_y(0).wait_recv()
            weight_y(1).wait_recv()

        number = len(pieces)

        @when(step, "f0", None)
        def _():
            for k in range(number):
                take_far(0, k)

        @when(step, "f1", None)
        def _():
            for k in range(number):
                take_far(1, k)

        @pl.when((step == last_step) & (keep_late == 0))
        def _():
            lax.fori_loop(0, 4 * waiting, return_held, 0)

        waves = number // 2
        extra = -(-(len(cot_pieces) - 4) // number)
        takes = [("f0", (k - number + 2) * 3 if k < number - 2 else 0) for k in range(number)]
        takes += [("fy0", 0)] * waves + [("f1", 0)] * (number - waves)
        for k, (name, shift) in enumerate(takes):
            @when(step, None, name, shift)
            def _():
                take_far(k // number, k % number)
                if k < number:
                    start_cot_pieces(4 + extra * k, 4 + extra * (k + 1))

        for h in range(2):
            @when(step, f"fy{h}", f"fy{h}")
            def _():
                for k in range(number):
                    far_y(h, k).wait_recv()

        w, t, n = order_at(step)

        def product(size):
            value = lax.dot_general(
                W[pl.ds(w, size)].reshape(size * half, W.shape[2]),
                C[t],
                (((1,), (1,)), ((), ())),
                preferred_element_type=jnp.float32,
            ).astype(jnp.bfloat16)
            for q in range(size):
                for part in range(2):
                    S[w + q, t, part] = value[
                        half * q : half * (q + 1), lanes * part : lanes * (part + 1)
                    ]

        @pl.when((step < tiles) & (n == 1))
        def _():
            product(1)

        @pl.when((step < tiles) & (n == 2))
        def _():
            product(2)

        for q in range(2):
            @pl.when((step < tiles) & (q < n) & (w // 4 != keep_late))
            def _():
                remote(
                    S.at[w + q, t], X.at[w % 4 + q, t], x_send, x_recv.at[w % 4 + q, t], twin
                ).start()

        back = jnp.maximum(step - lag, 0)
        w2, t2, n2 = order_at(back)

        for q in range(2):
            @pl.when((step >= lag) & (step < tiles + lag) & (q < n2) & (w2 // 4 == keep_late))
            def _():
                mine, slot = w2 + q, w2 % 4 + q
                remote(
                    S.at[mine, t2], X.at[slot, t2], x_send, x_recv.at[slot, t2], twin
                ).wait_recv()
                total = S[mine, t2].astype(jnp.float32) + X[slot, t2].astype(jnp.float32)
                S[mine, t2] = total.astype(jnp.bfloat16)
                rows = sum_rows(slot)
                i = t2 % count

                @pl.when(t2 < count)
                def _():
                    R[i, rows, :] = total[0].astype(jnp.bfloat16)
                    remote(S.at[mine, t2, 1], R.at[i, rows], r_send, r_recv.at[i], core).start()

                @pl.when((t2 >= count) & ((keep_late == 1) | (t2 >= count + waiting)))
                def _():
                    return_far(mine, t2, rows)

        return carry

    lax.fori_loop(0, max(lengths) + lag, body, 0)

    spread_y().wait_recv()
    spread_c().start()
    spread_c().wait_recv()
    for j in range(feature_blocks):
        for m in range(3):
            GDV[m, :, pl.ds(j * lanes, lanes)] = F[m * feature_blocks + j].astype(jnp.float32)
    for m, ref in enumerate((GQ, GK, GV)):
        low, high = columns[m]
        for j in range((high - low) // lanes):
            ref[:, pl.ds(j * lanes, lanes)] = F[first + low // lanes + j].astype(jnp.float32)
    part = pl.ds(0, 3 * R.shape[1] // 4)
    stores = [
        pltpu.make_async_copy(source, target, grad_sem.at[k])
        for k, (source, target) in enumerate(
            zip((GDV, GQ, GK, GV), (grad_down, grad_up_q, grad_up_k, grad_up_v))
        )
    ]
    for i in range(count):
        inverse_out[pl.ds(i * lanes, lanes), :] = INV[i]
    for store in stores:
        store.start()
    for i in range(count):
        rows = pl.ds(i * lanes, lanes)
        remote(R.at[i, part], R.at[i, part], r_send, r_recv.at[i], core).wait_recv()
        inverse = INV[i]

        def gained_block(j, carry, i=i, rows=rows, inverse=inverse):
            cols = pl.ds(pl.multiple_of(j * lanes, lanes), lanes)
            back = R[i, cols, :].astype(jnp.float32).T
            back = back + adapter_scale * jnp.dot(
                LO[i], D[:, cols], preferred_element_type=jnp.float32
            )
            gained = GA[:, cols] * back
            B[rows, cols] = gained
            return carry + gained * (T[rows, cols].astype(jnp.float32) * inverse)

        total = lax.fori_loop(
            0, feature_blocks, gained_block, jnp.zeros((lanes, lanes), jnp.float32), unroll=11
        )
        I[i] = jnp.broadcast_to(jnp.sum(total.T, axis=0, keepdims=True), (8, lanes))
        inner_rows(i).start()
        stores.append(pltpu.make_async_copy(B.at[rows], out.at[rows], store_sem.at[i]))
        stores[-1].start()
    for i in range(count):
        rows = pl.ds(i * lanes, lanes)
        inner_rows(i).wait_recv()
        inner = (I[i, pl.ds(0, 1)] + IR[i, pl.ds(0, 1)]) / full_width
        inner_out[rows, :] = jnp.broadcast_to(inner, (lanes, lanes)).T

    results = remote(R.at[:, part], R.at[:, part], r_send, r_recv.at[0], core)
    results.wait_send()
    own = C.at[pl.ds(0, count), lower]
    remote(own, own, cc_send, cc_recv.at[0], core).wait_send()
    remote(own, own, cz_send, cz_recv.at[0], core).wait_send()
    remote(own, own, zc_send, zc_recv.at[0], core).wait_send()
    two = W.at[pl.ds(0, 2)]
    remote(two, two, y_send, y_recv.at[0], core).wait_send()

    @pl.when(is_inner == 0)
    def _():
        remote(two, two, far_send, far_recv.at[0, 0], core).wait_send()

    remote(two, two, fy_send, fy_recv.at[0, 0], core).wait_send()
    four = S.at[pl.ds(0, 4)]
    remote(four, four, x_send, x_recv.at[0, 0], core).wait_send()
    pair_rows().wait_send()
    remote(I, I, i_send, i_recv.at[0], twin).wait_send()
    grads_core().wait_send()
    grads_row().wait_send()
    three = H.at[pl.ds(0, 3 * piece)]
    remote(three, three, gz_send, gz_recv.at[0], core).wait_send()
    three = F.at[pl.ds(0, 3 * piece)]
    remote(three, three, ga_send, ga_recv.at[0], core).wait_send()
    spread_y().wait_send()
    spread_c().wait_send()
    for store in stores:
        store.wait()


token_lanes = 128


def final_kernel(gained, tokens, inner, inverse, *refs):
    grads, (out, *grad_outs) = refs[:4], refs[4:]

    @pl.when(pl.program_id(0) == 0)
    def _():
        for source, target in zip(grads, grad_outs):
            target[...] = source[...]

    scale = inverse[:, :1]
    unit = tokens[...].astype(jnp.float32) * scale
    out[...] = (scale * (gained[...] - unit * inner[:, :1])).astype(out.dtype)


def grid_fits(weights, cotangents, tokens, rank):
    rows = weights[0].shape[0]
    tokens_here, owned = tokens.shape
    count = tokens_here // token_lanes
    aligned = all(c.shape[1] % token_lanes == 0 for c in cotangents) and owned % token_lanes == 0
    return (
        aligned and rows % 32 == 0 and tokens_here % token_lanes == 0
        and count in (3, 4) and rank == 16 and owned == 8 * rows
    )


def grid_step(tokens, gain, weights, adapters, ups, cotangents):
    rows = weights[0].shape[0]
    tokens_here, owned = tokens.shape
    full_width = gain.shape[0]
    rank = adapters.shape[1]
    depth = sum(w.shape[1] for w in weights)
    half = rows // 2
    lanes = token_lanes
    count = tokens_here // lanes
    number = len(piece_rows(half))
    scale = adapter_scale / math.sqrt(tokens_here * lax.axis_size("fsdp"))
    grad_blocks = 16 * -(-(3 * owned + depth) // (16 * lanes))
    share = grad_blocks // 2
    DMA = pltpu.SemaphoreType.DMA
    f32, bf16 = jnp.float32, jnp.bfloat16
    vmem = pl.BlockSpec(memory_space=pltpu.VMEM)
    gained, inner, inverse, *grads = pl.pallas_call(
        functools.partial(grid_kernel, (full_width, owned, rank, scale)),
        out_shape=(
            jax.ShapeDtypeStruct(tokens.shape, f32),
            jax.ShapeDtypeStruct((tokens_here, lanes), f32),
            jax.ShapeDtypeStruct((tokens_here, lanes), f32),
            jax.ShapeDtypeStruct((3, rank, owned), f32),
        ) + tuple(jax.ShapeDtypeStruct((rank, c.shape[1]), f32) for c in cotangents),
        in_specs=[pl.BlockSpec(memory_space=pl.ANY)] * 12,
        out_specs=(pl.BlockSpec(memory_space=pl.ANY),) + (vmem,) * 2
        + (pl.BlockSpec(memory_space=pl.ANY),) * 4,
        scratch_shapes=[
            pltpu.VMEM((8, half, depth), bf16),
            pltpu.VMEM((2 * count, 2 * lanes, depth), bf16),
            pltpu.VMEM((8, 2 * count, 2, half, lanes), bf16),
            pltpu.VMEM((4, 2 * count, 2, half, lanes), bf16),
            pltpu.VMEM((count, 8 * rows, lanes), bf16),
            pltpu.VMEM((tokens_here, owned), bf16),
            pltpu.VMEM((full_width // lanes, lanes), f32),
            pltpu.VMEM((1, owned), f32),
            pltpu.VMEM((lanes, depth), bf16),
            pltpu.VMEM((lanes, owned), bf16),
            pltpu.VMEM((3, lanes, owned), bf16),
            pltpu.VMEM((count, lanes, lanes), f32),
            pltpu.VMEM((count, lanes, lanes), f32),
            pltpu.VMEM((count, lanes, lanes), f32),
            pltpu.VMEM((count, lanes, lanes), bf16),
            pltpu.VMEM((lanes, tokens_here), bf16),
            pltpu.VMEM((tokens_here, owned), bf16),
            pltpu.VMEM((tokens_here, owned), f32),
            pltpu.VMEM((count, 8, lanes), f32),
            pltpu.VMEM((count, 8, lanes), f32),
            pltpu.VMEM((grad_blocks, rank, lanes), f32),
            pltpu.VMEM((share, rank, lanes), f32),
            pltpu.VMEM((share // 2, rank, lanes), f32),
            pltpu.VMEM((share // 2, rank, lanes), bf16),
            pltpu.VMEM((3, share // 8, rank, lanes), bf16),
            pltpu.VMEM((grad_blocks, rank, lanes), bf16),
            pltpu.VMEM((3, rank, owned), f32),
            *[pltpu.VMEM((rank, c.shape[1]), f32) for c in cotangents],
            DMA((4,)),
            DMA((2, 3)), DMA((count, 3)), DMA((8,)), DMA((count,)),
            DMA, DMA, DMA, DMA((count,)),
            DMA, DMA, DMA, DMA, DMA, DMA((3,)), DMA, DMA((3,)), DMA, DMA, DMA, DMA,
            DMA, DMA((count,)), DMA, DMA((count,)), DMA, DMA((count,)),
            DMA, DMA((2,)), DMA, DMA((2, number)), DMA, DMA((2, number)),
            DMA, DMA((4, 2 * count)), DMA, DMA((count,)),
        ],
        compiler_params=pltpu.CompilerParams(
            collective_id=0, has_side_effects=True, vmem_limit_bytes=60 * 1024 * 1024
        ),
        cost_estimate=pl.CostEstimate(
            flops=2 * 16 * rows * tokens_here * depth, bytes_accessed=2 * 8 * rows * depth,
            transcendentals=0,
        ),
        name="grid",
    )(*cotangents, *weights, tokens, gain.reshape(full_width // lanes, lanes), adapters, *ups)
    step_rows = tokens_here // 2

    def by_rows(width):
        return pl.BlockSpec((step_rows, width), lambda i: (i, 0))

    whole = [pl.BlockSpec(g.shape, lambda i, k=len(g.shape): (0,) * k) for g in grads]
    return pl.pallas_call(
        final_kernel,
        grid=(tokens_here // step_rows,),
        out_shape=(jax.ShapeDtypeStruct(tokens.shape, bf16),)
        + tuple(jax.ShapeDtypeStruct(g.shape, f32) for g in grads),
        in_specs=[by_rows(owned), by_rows(owned), by_rows(lanes), by_rows(lanes), *whole],
        out_specs=(by_rows(owned), *whole),
        cost_estimate=pl.CostEstimate(
            flops=4 * tokens_here * owned, bytes_accessed=8 * tokens_here * owned, transcendentals=0
        ),
        name="final",
    )(gained, tokens, inner, inverse, *grads)


def shards(
    tokens,
    gain,
    query_projection_weight,
    key_projection_weight,
    value_projection_weight,
    adapter_down_factors,
    query_adapter_up,
    key_adapter_up,
    value_adapter_up,
    query_cotangent,
    key_cotangent,
    value_cotangent,
):
    return device_work(
        tokens,
        gain,
        (query_projection_weight, key_projection_weight, value_projection_weight),
        adapter_down_factors,
        (query_adapter_up, key_adapter_up, value_adapter_up),
        (query_cotangent, key_cotangent, value_cotangent),
    )


def device_work(tokens, gain, weights, adapter_down_factors, ups, cots):
    fsdp_size = lax.axis_size("fsdp")
    tp_size = lax.axis_size("tp")
    tp_index = lax.axis_index("tp")
    row_count, owned = tokens.shape
    full_width = gain.shape[0]
    rank = adapter_down_factors.shape[1]
    if tp_size == 2 and fsdp_size == 16 and grid_fits(weights, cots, tokens, rank):
        return grid_step(tokens, gain, weights, adapter_down_factors, ups, cots)

    def tp_sum(value):
        if tp_size != 2:
            return lax.psum(value, "tp")
        with jax.named_scope("pair_sum"):
            return value + lax.ppermute(value, "tp", [(0, 1), (1, 0)])

    wide = tokens.astype(jnp.float32)
    gain_own = lax.dynamic_slice_in_dim(gain, tp_index * owned, owned, 0)
    down = lax.dynamic_slice_in_dim(adapter_down_factors, tp_index * owned, owned, 2)
    down = down.reshape(3 * rank, owned)
    low_in = lax.dot_general(
        wide * gain_own[None, :],
        down.astype(jnp.float32),
        (((1,), (1,)), ((), ())),
        precision=lax.Precision.HIGHEST,
    )
    low_out = jnp.concatenate([transposed_product(c, u) for c, u in zip(cots, ups)], axis=1)
    squares = jnp.sum(wide * wide, axis=1, keepdims=True)
    small = tp_sum(jnp.concatenate([squares, low_in, low_out], axis=1))
    inverse = lax.rsqrt(small[:, :1] / full_width + norm_eps)
    in_low = (small[:, 1 : 1 + 3 * rank] * inverse).astype(jnp.bfloat16)
    out_low = small[:, 1 + 3 * rank :].astype(jnp.bfloat16)
    unit_rows = wide * inverse
    normed = (unit_rows * gain_own[None, :]).astype(jnp.bfloat16)
    scale = adapter_scale / math.sqrt(row_count * fsdp_size)

    def token_product(left, right):
        return scale * lax.dot_general(
            left, right, (((0,), (0,)), ((), ())), preferred_element_type=jnp.float32
        )

    down_local = token_product(out_low, normed)
    up_local = [
        token_product(in_low[:, rank * m : rank * (m + 1)], cots[m]) for m in range(3)
    ]
    small_work = tuple(down_local[rank * m : rank * (m + 1)] for m in range(3)) + tuple(up_local)
    back = plain_back(weights, cots, full_width)
    grads = lax.psum(jnp.concatenate(small_work, axis=1), "fsdp")
    grad_down = jnp.stack([grads[:, owned * m : owned * (m + 1)] for m in range(3)])
    ends = [3 * owned]
    for cot in cots:
        ends.append(ends[-1] + cot.shape[1])
    up_q, up_k, up_v = [grads[:, low:high] for low, high in zip(ends[:-1], ends[1:])]

    back = back + adapter_scale * jnp.dot(out_low, down, preferred_element_type=jnp.float32)
    gained = gain_own[None, :] * back
    inner = tp_sum(jnp.sum(gained * unit_rows, axis=1, keepdims=True)) / full_width
    grad_tokens = (inverse * (gained - unit_rows * inner)).astype(jnp.bfloat16)
    return (grad_tokens, grad_down, up_q, up_k, up_v)


def solution(mesh):
    in_specs = (
        P("fsdp", "tp"),
        P(),
        P("fsdp", "tp"),
        P("fsdp", "tp"),
        P("fsdp", "tp"),
        P(),
        P(None, "tp"),
        P(None, "tp"),
        P(None, "tp"),
        P("fsdp", "tp"),
        P("fsdp", "tp"),
        P("fsdp", "tp"),
    )
    out_specs = (P("fsdp", "tp"), P(None, None, "tp"), P(None, "tp"), P(None, "tp"), P(None, "tp"))
    step = jax.shard_map(shards, mesh=mesh, in_specs=in_specs, out_specs=out_specs, check_vma=False)
    return step
```
